32 devices in a mesh: space: 16 (over z, y, core), probe: 2 (over x).
Axes of the slice: x: 2, y: 2, z: 4, core: 2. Of those that a mesh axis runs over, the one named last changes fastest.
Arguments:
- positions: bfloat16 [128, 3, 32], P('space'), may hold values from -4.3125 to 4.3125
- probes: bfloat16 [128, 512, 128], P('space', 'probe'), may hold values from -4 to 4
- neighbours: int32 [128, 15], P('space'), may hold values from -1 to 127, as said below
Outputs:
- density: bfloat16 [128, 128, 15, 128], P('probe', 'space')
- forces: float32 [128, 3, 32], P('space')
The draws below stay inside these ranges and needn't reach their ends.
Inputs may be any that keep to these rules, and one draw needn't show every extreme that they name: `neighbours`: slot 0 of each cluster names the cluster itself. Clusters are held 8 to an index of space in order; every other entry is -1 or a cluster held by the same index of space or by the index one before or one after it, cyclically. The clusters named in one row are distinct.
All inputs are finite; a program needn't handle non-finite values.
Results may differ from the reference program's by a relative error of at most 0.0018.
The reference program's roundings to bfloat16 on the way (of `scaled`, `one_half` and `mixture`) count: a program that leaves them out, or rounds other values in their place, can miss the bound.
Values may be sent and summed in bfloat16 or wider, within the bound.
A program may use at most 64 MiB of HBM per device.

```python
import jax
import jax.numpy as jnp
from jax import lax

ATOMS_C = 32
ORB = 128
NBLK = 15
PROBES = 512
CL_DEV = 8
CLUSTERS = 128
N_SPACE = 16


BOX_EDGE = 8.6


def draw_positions(key, part):
    coords = jax.random.uniform(key, (CLUSTERS, 3, ATOMS_C), jnp.float32, -0.5, 0.5) * BOX_EDGE
    return coords.astype(jnp.bfloat16)


def draw_neighbours(key, part):
    candidates = 3 * CL_DEV
    scores = jax.random.randint(key, (CLUSTERS, candidates), 0, 2 ** 20) * candidates
    scores = scores + jnp.arange(candidates, dtype=jnp.int32)[None, :]
    own_ids = jnp.arange(CLUSTERS, dtype=jnp.int32)
    device = own_ids // CL_DEV
    self_place = CL_DEV + own_ids % CL_DEV
    scores = jnp.where(jnp.arange(candidates, dtype=jnp.int32)[None, :] == self_place[:, None], 2 ** 30, scores)
    chosen = jnp.argsort(scores, axis=1)[:, :NBLK - 1].astype(jnp.int32)
    others = (device[:, None] + chosen // CL_DEV - 1) % N_SPACE * CL_DEV + chosen % CL_DEV
    surface = device[:, None] < max(1, N_SPACE // 4)
    coin = jax.random.randint(jax.random.fold_in(key, 7), (CLUSTERS, NBLK - 1), 0, 2)
    others = jnp.where(surface & (coin == 0), -1, others)
    return jnp.concatenate([own_ids[:, None], others], axis=1).astype(jnp.int32)


def shard_levels(key, extent, cuts, least, top_value):
    factor_of = 1.0
    for position, parts in cuts:
        steps = jax.random.uniform(jax.random.fold_in(jax.random.fold_in(key, 6), position), (parts,), jnp.float32, least / len(cuts), top_value / len(cuts))
        factor_of = factor_of * jnp.repeat(jnp.exp(steps), extent[position] // parts).reshape((-1,) + (1,) * (len(extent) - 1 - position))
    return factor_of


def gaussian(stream_key, extent, deviation, limit, split=(), held_as=jnp.bfloat16):
    factor_of = shard_levels(stream_key, extent, split, -0.22, 0.18) if split else 1.0
    values = jax.random.normal(stream_key, extent, jnp.float32) * deviation * factor_of
    return jnp.minimum(jnp.maximum(values, -limit), limit).astype(held_as)


def setup_inputs(seed: int = 0) -> dict:
    splits = jax.random.split(jax.random.key(seed), 4)
    positions = draw_positions(jax.random.fold_in(splits[3], 71), 0)
    probes = gaussian(splits[1], (CLUSTERS, PROBES, ORB), 1.0, 4.0, ((0, 16), (1, 2)))
    neighbours = draw_neighbours(jax.random.fold_in(splits[3], 71), 0)
    return {"positions": positions, "probes": probes, "neighbours": neighbours}


SS_SIGMA = -1.938
SP_SIGMA = 1.745
PP_SIGMA = 3.05
PP_PI = -1.075
BOND_LENGTH = 2.35
SOFT_SQUARE = 0.25
CELL_EDGE = 10.86
COEFF_ZERO = 0.6
COEFF_ONE = -0.7
COEFF_TWO = 0.45

def offsets():
    half = CELL_EDGE / 2.0
    table = [[0.0, 0.0, 0.0]]
    for sign_x in (-1.0, 1.0):
        for sign_y in (-1.0, 1.0):
            for sign_z in (-1.0, 1.0):
                table.append([sign_x * half, sign_y * half, sign_z * half])
    for axis_pick in range(3):
        for sign_a in (1.0, -1.0):
            entry = [0.0, 0.0, 0.0]
            entry[axis_pick] = sign_a * CELL_EDGE
            table.append(entry)
    return jnp.array(table, dtype=jnp.float32)

def build_rows(own_pos, col_pos, start_row, row_count):
    atom_count = own_pos.shape[-1]
    row_index = start_row + jnp.arange(row_count, dtype=jnp.int32)
    orbital = row_index // atom_count
    atom_index = row_index % atom_count
    atom_pick = (jnp.arange(atom_count, dtype=jnp.int32)[:, None] == atom_index[None, :]).astype(jnp.float32)
    weights = (jnp.arange(4, dtype=jnp.int32)[:, None] == orbital[None, :]).astype(jnp.float32)
    row_pos = jnp.dot(own_pos, atom_pick, precision=lax.Precision.HIGHEST)
    offset_vec = col_pos[:, None, :] - row_pos[:, :, None]
    dist_square = lax.optimization_barrier(jnp.sum(offset_vec * offset_vec, axis=0)) + SOFT_SQUARE
    cosine = offset_vec / jnp.sqrt(dist_square)
    radial = jnp.exp(1.0 - dist_square / (BOND_LENGTH * BOND_LENGTH))
    projected = lax.optimization_barrier(jnp.sum(weights[1:, :, None] * cosine, axis=0))
    s_orbital = weights[0][:, None]
    columns = [(s_orbital * SS_SIGMA - projected * SP_SIGMA) * radial]
    for direction in range(3):
        columns.append((s_orbital * cosine[direction] * SP_SIGMA + projected * cosine[direction] * (PP_SIGMA - PP_PI) + weights[1 + direction][:, None] * PP_PI) * radial)
    return jnp.stack(columns, axis=1).reshape(row_count, 4 * atom_count)

def cluster_blocks(own_pos, near_pos, present, start_row, row_count):
    made = jax.vmap(build_rows, in_axes=(None, 0, None, None))(own_pos, near_pos, start_row, row_count)
    return made * present.astype(jnp.float32)[:, None, None]

def reference(positions, probes, neighbours):
    coords = positions.astype(jnp.float32)
    cluster_count = coords.shape[0]
    orbitals = 4 * coords.shape[2]
    total_probes = probes.shape[1]
    slot_count = neighbours.shape[1]
    present = neighbours >= 0
    target = jnp.where(present, neighbours, 0).astype(jnp.int32)
    shifts = offsets()
    cluster_ids = jnp.arange(cluster_count, dtype=jnp.int32)

    def blocks_of(cluster):
        beside_all = coords[target[cluster]] + shifts[:, :, None]
        return cluster_blocks(coords[cluster], beside_all, present[cluster], 0, orbitals)
    row_peaks = lax.map(lambda cluster: jnp.max(lax.optimization_barrier(jnp.sum(jnp.abs(blocks_of(cluster)), axis=(0, 2)))), cluster_ids)
    spectral = jnp.max(row_peaks)

    def apply_all(vectors):

        def one_cluster(cluster):
            rounded = lax.optimization_barrier((blocks_of(cluster) / spectral).astype(jnp.bfloat16))
            scaled = rounded.astype(jnp.float32)
            nearby = vectors[target[cluster]].astype(jnp.float32)
            return jnp.einsum('kpj,kij->pi', nearby, scaled)
        return lax.map(one_cluster, cluster_ids)
    probe_wide = probes.astype(jnp.float32)
    term_one = apply_all(probes)
    one_half = term_one.astype(jnp.bfloat16)
    term_two = 2.0 * apply_all(one_half) - probe_wide
    mixture = (COEFF_ZERO * probe_wide + COEFF_ONE * term_one + COEFF_TWO * term_two).astype(jnp.bfloat16)

    def sample_of(cluster):
        nearby = probes[target[cluster]].astype(jnp.float32)
        alive = present[cluster].astype(jnp.float32)
        sample = jnp.einsum('pi,kpj->kij', mixture[cluster].astype(jnp.float32), nearby) * alive[:, None, None]

        def energy(own_pos, near_pos):
            made = cluster_blocks(own_pos, near_pos + shifts[:, :, None], present[cluster], 0, orbitals)
            return jnp.sum(made * sample) / total_probes
        own_grad, near_grad = jax.grad(energy, argnums=(0, 1))(coords[cluster], coords[target[cluster]])
        scaled_out = (sample / jnp.sqrt(jnp.float32(total_probes))).astype(jnp.bfloat16)
        return (scaled_out, own_grad, near_grad)
    density, own_grad, near_grad = lax.map(sample_of, cluster_ids)
    spread = jax.ops.segment_sum(near_grad.reshape(cluster_count * slot_count, 3, coords.shape[2]), target.reshape(-1), num_segments=cluster_count)
    forces = -(own_grad + spread)
    return (jnp.transpose(density, (2, 0, 1, 3)), forces)
```

```python
import functools

import jax
import jax.numpy as jnp
from jax import lax
from jax.experimental import pallas as pl
from jax.experimental.pallas import tpu as pltpu
from jax.sharding import PartitionSpec as P

SS_SIGMA = -1.938
SP_SIGMA = 1.745
PP_SIGMA = 3.05
PP_PI = -1.075
PP_DIFF = PP_SIGMA - PP_PI
BOND_LENGTH = 2.35
SOFT_SQUARE = 0.25
CELL_EDGE = 10.86
COEFF_ZERO = 0.6
COEFF_ONE = -0.7
COEFF_TWO = 0.45
MESH = pl.DeviceIdType.MESH
LANES = 128
F32 = jnp.float32
BF16 = jnp.bfloat16


def offsets():
    half = CELL_EDGE / 2.0
    table = [(0.0, 0.0, 0.0)]
    for x in (-1.0, 1.0):
        for y in (-1.0, 1.0):
            for z in (-1.0, 1.0):
                table.append((x * half, y * half, z * half))
    for axis in range(3):
        for sign in (1.0, -1.0):
            entry = [0.0, 0.0, 0.0]
            entry[axis] = sign * CELL_EDGE
            table.append(tuple(entry))
    return table


SHIFTS = offsets()


def kernel(
    sizes,
    neighbours_ref,
    positions_ref,
    probes_ref,
    dens_ref,
    force_ref,
    names_ref,
    slot_ref,
    alive_ref,
    wanted_ref,
    raw_pos,
    posc_ref,
    near,
    rest,
    near_pos,
    ham,
    scaled,
    pair,
    top_out,
    top_in,
    slope,
    first,
    one_t,
    mix,
    row_mix,
    dense,
    stage,
    col_force,
    row_force,
    pull,
    arrived,
    local_sem,
    pos_s,
    pos_r,
    probe_s,
    probe_r,
    own_s,
    own_r,
    fwd_s,
    fwd_r,
    chip_s,
    chip_r,
    max_s,
    max_r,
    one_s,
    one_r,
    mix_s,
    mix_r,
    pull_s,
    pull_r,
):
    space, wide, count, atoms, slots, span, share = sizes
    orbitals = 4 * atoms
    total = span * wide
    s = lax.axis_index("space")
    q = lax.axis_index("probe")
    up = lax.rem(s + 1, space)
    down = lax.rem(s + space - 1, space)
    before, own, after = pl.ds(0, count), pl.ds(count, count), pl.ds(2 * count, count)
    core = lax.rem(s, 2)
    mate = s + 1 - 2 * core
    far_side = pl.ds(core * (2 * count), count)

    def send(src, dst, ss, rs, to_space, to_probe):
        return pltpu.make_async_remote_copy(
            src_ref=src,
            dst_ref=dst,
            send_sem=ss,
            recv_sem=rs,
            device_id={"space": to_space, "probe": to_probe},
            device_id_type=MESH,
        )

    steps = space.bit_length() - 1
    partners = []
    for j in range(steps):
        bit = lax.rem(lax.div(s, 2**j), 2)
        partners.append(s + 2**j * (1 - 2 * bit))

    barrier = pltpu.get_barrier_semaphore()

    def greet(to_space, to_probe):
        pl.semaphore_signal(
            barrier,
            inc=1,
            device_id={"space": to_space, "probe": to_probe},
            device_id_type=MESH,
        )

    for to in partners + [up, down]:
        greet(to, q)
    for e in range(1, wide):
        for to in (s, up, down):
            greet(to, lax.rem(q + e, wide))

    loads = [
        pltpu.make_async_copy(src, dst, local_sem.at[i])
        for i, (src, dst) in enumerate(
            [
                (positions_ref, raw_pos.at[1]),
                (neighbours_ref, names_ref),
                (neighbours_ref, wanted_ref),
                (probes_ref, near.at[own]),
            ]
        )
    ]
    for load in loads:
        load.start()
    pl.semaphore_wait(barrier, steps + 2 + 3 * (wide - 1))

    pos_up = send(positions_ref, raw_pos.at[0], pos_s.at[0], pos_r.at[0], up, q)
    pos_down = send(positions_ref, raw_pos.at[2], pos_s.at[1], pos_r.at[1], down, q)
    pos_up.start()
    pos_down.start()
    probe_up = send(probes_ref, near.at[before], probe_s.at[0], probe_r.at[0], up, q)
    probe_down = send(probes_ref, near.at[after], probe_s.at[1], probe_r.at[1], down, q)
    probe_up.start()
    probe_down.start()
    own_out = []
    for e in range(1, wide):
        copy = send(
            probes_ref,
            rest.at[e - 1, own],
            own_s.at[e - 1],
            own_r.at[e - 1],
            s,
            lax.rem(q + e, wide),
        )
        copy.start()
        own_out.append(copy)

    def fold(x):
        return (
            x
            + pltpu.roll(x, atoms, 1)
            + pltpu.roll(x, 2 * atoms, 1)
            + pltpu.roll(x, 3 * atoms, 1)
        )

    def spread(part):
        rows = pl.ds(part * count, count)
        for m in range(3):
            near_pos[m, rows, :atoms] = raw_pos[part, m].astype(F32)
            near_pos[m, rows] = fold(jnp.where(narrow, near_pos[m, rows], 0.0))

    for load in loads[:3]:
        load.wait()
    narrow = lax.broadcasted_iota(jnp.int32, (count, orbitals), 1) < atoms
    spread(1)
    for m in range(3):
        tall = jnp.transpose(near_pos[m, own])
        for c in range(count):
            posc_ref[c, m] = jnp.broadcast_to(tall[:atoms, c : c + 1], (atoms, orbitals))

    def find_slots(c, carry):
        for k in range(slots):
            name = names_ref[c, k]
            held = jnp.maximum(name, 0)
            place = lax.rem(lax.div(held, count) - s + 1 + space, space) * count
            place = place + lax.rem(held, count)
            slot_ref[c, k] = jnp.where(name >= 0, jnp.minimum(place, 3 * count - 1), count)
            alive_ref[c, k] = jnp.where(name >= 0, 1.0, 0.0)
        return carry

    lax.fori_loop(0, count, find_slots, 0)
    pos_up.wait_recv()
    spread(0)
    pos_down.wait_recv()
    spread(2)

    lane = lax.broadcasted_iota(jnp.int32, (atoms, orbitals), 1)
    group = lane // atoms
    is_s = group == 0
    is_p = [group == 1, group == 2, group == 3]
    pp = [jnp.where(m, PP_PI, 0.0).astype(F32) for m in is_p]

    def peak_of(c, peak):
        rows = [posc_ref[c, m] for m in range(3)]
        sums = [jnp.zeros((atoms, orbitals), F32) for _ in range(4)]
        for k in range(0, slots, 4):
            picked = range(k, min(k + 4, slots))
            alive = jnp.zeros((1, orbitals), F32)
            column = [jnp.zeros((1, orbitals), F32) for _ in range(3)]
            for i, t in enumerate(picked):
                here = group[:1] == i
                alive = jnp.where(here, alive_ref[c, t], alive)
                place = slot_ref[c, t]
                for m in range(3):
                    column[m] = jnp.where(
                        here, near_pos[m, pl.ds(place, 1), :] + SHIFTS[t][m], column[m]
                    )
            d = [column[m] - rows[m] for m in range(3)]
            square = d[0] * d[0] + d[1] * d[1] + d[2] * d[2] + SOFT_SQUARE
            inv = lax.rsqrt(square)
            u = [jnp.abs(x) * inv for x in d]
            g = jnp.exp(1.0 - square * (1.0 / (BOND_LENGTH * BOND_LENGTH))) * alive
            sums[0] = sums[0] + g * ((u[0] + u[1] + u[2]) * SP_SIGMA - SS_SIGMA)
            for a in range(3):
                others = u[(a + 1) % 3] + u[(a + 2) % 3]
                value = u[a] * (others * PP_DIFF + SP_SIGMA)
                value = value + jnp.abs(u[a] * u[a] * PP_DIFF + PP_PI)
                sums[1 + a] = sums[1 + a] + g * value
        for a in range(4):
            peak = jnp.maximum(peak, jnp.sum(sums[a], axis=1, keepdims=True))
        return peak

    def build(c, carry):
        rows = [posc_ref[c, m] for m in range(3)]
        for k in range(slots):
            place = slot_ref[c, k]
            alive = alive_ref[c, k]
            d = [
                (near_pos[m, pl.ds(place, 1), :] + SHIFTS[k][m]) - rows[m] for m in range(3)
            ]
            square = d[0] * d[0] + d[1] * d[1] + d[2] * d[2] + SOFT_SQUARE
            inv = lax.rsqrt(square)
            l = [x * inv for x in d]
            g = jnp.exp(1.0 - square * (1.0 / (BOND_LENGTH * BOND_LENGTH))) * alive
            beta = jnp.where(
                is_s, 0.0, jnp.where(is_p[0], l[0], jnp.where(is_p[1], l[1], l[2]))
            )
            coef_s = jnp.where(is_s, SS_SIGMA, SP_SIGMA * beta)
            coef_p = jnp.where(is_s, -SP_SIGMA, PP_DIFF * beta)
            parts = [coef_s * g] + [(l[m] * coef_p + pp[m]) * g for m in range(3)]
            for a in range(4):
                ham[c, a * atoms : (a + 1) * atoms, k * orbitals : (k + 1) * orbitals] = parts[a]
            pair[c, k, 0] = jnp.zeros_like(g)
            for m in range(3):
                pair[c, k, 1 + m] = l[m]
            pair[c, k, 4] = beta
            pair[c, k, 5] = g * inv
            pair[c, k, 6] = g * (square * inv) * (2.0 / (BOND_LENGTH * BOND_LENGTH))
        return carry

    peak = lax.fori_loop(0, count, peak_of, jnp.zeros((atoms, 1), F32))
    top = jnp.broadcast_to(jnp.max(peak, axis=0, keepdims=True), (8, LANES))
    order = [0] + list(range(2, steps)) + ([1] if steps > 1 else [])
    done = 0
    for t, j in enumerate(order):
        top_out[j] = top
        copy = send(top_out.at[j], top_in.at[j], max_s.at[j], max_r.at[j], partners[j], q)
        copy.start()
        until = count if t == len(order) - 1 else count * (t + 1) // len(order)
        lax.fori_loop(done, until, build, 0)
        done = until
        copy.wait()
        top = jnp.maximum(top, top_in[j])
    shrink = 1.0 / top[0:1]

    loads[3].wait()
    probe_up.wait_recv()
    probe_down.wait_recv()
    fwd_out = []
    for e in range(1, wide):
        copy = send(
            near.at[far_side],
            rest.at[e - 1, far_side],
            fwd_s.at[e - 1],
            fwd_r.at[e - 1],
            s,
            lax.rem(q + e, wide),
        )
        copy.start()
        fwd_out.append(copy)

    def one_copies(c):
        return (
            send(one_t.at[count + c], one_t.at[c], one_s.at[0, c], one_r.at[0, c], up, q),
            send(
                one_t.at[count + c], one_t.at[2 * count + c], one_s.at[1, c], one_r.at[1, c], down, q
            ),
        )

    def term_one(c, carry):
        for k in range(slots):
            part = pl.ds(k * orbitals, orbitals)
            scaled[c, :, part] = (ham[c, :, part] * shrink).astype(BF16)
        right = jnp.concatenate([near[slot_ref[c, k]] for k in range(slots)], axis=1)
        term = lax.dot_general(
            scaled[c], right, (((1,), (1,)), ((), ())), preferred_element_type=F32
        )
        first[c] = term
        one_t[count + c] = term.astype(BF16)
        for copy in one_copies(c):
            copy.start()
        return carry

    lax.fori_loop(0, count, term_one, 0)

    chip_out = []
    for e in range(1, wide):
        own_out[e - 1].wait_recv()
        copy = send(
            rest.at[e - 1, own],
            rest.at[e - 1, far_side],
            chip_s.at[e - 1],
            chip_r.at[e - 1],
            mate,
            q,
        )
        copy.start()
        chip_out.append(copy)

    height = min(atoms, share)
    turns = share // height
    start_atom = lax.rem(q * share, atoms)
    rows = pl.ds(pl.multiple_of(start_atom, height), height)
    s_mask = jnp.where(is_s[:height], 1.0, 0.0).astype(F32)
    p_mask = [jnp.where(m[:height], 1.0, 0.0).astype(F32) for m in is_p]
    row_iota = lax.broadcasted_iota(jnp.int32, (height, orbitals), 0) + start_atom
    hit = jnp.where(row_iota == lax.rem(lane[:height], atoms), 1.0, 0.0).astype(F32)
    scale = 1.0 / float(total) ** 0.5

    def slopes(c, carry):
        for t in range(turns):
            kind = (q * share) // atoms + t
            ws = jnp.where(kind == 0, 1.0, 0.0).astype(F32)
            wr = [jnp.where(kind == m + 1, 1.0, 0.0).astype(F32) for m in range(3)]
            wv = PP_PI * (wr[0] * p_mask[0] + wr[1] * p_mask[1] + wr[2] * p_mask[2])
            wv = wv + (ws * SS_SIGMA) * s_mask
            for k in range(slots):
                alpha = pair[c, k, kind, rows, :]
                beta = pair[c, k, 4, rows, :]
                lean = pair[c, k, 5, rows, :]
                c_one = PP_DIFF * alpha + ws * SP_SIGMA
                c_two = PP_DIFF * beta - SP_SIGMA * s_mask
                cross = alpha * c_two
                bracket = (ws * SP_SIGMA) * beta + cross + wv
                x = lean * c_one
                y = lean * c_two
                drag = lean * (c_one * beta + cross) + pair[c, k, 6, rows, :] * bracket
                for m in range(3):
                    slope[c, k, m, t * height : (t + 1) * height] = (
                        x * p_mask[m] + y * wr[m] - drag * pair[c, k, 1 + m, rows, :]
                    )
        return carry

    lax.fori_loop(0, count, slopes, 0)

    def wait_one(c, carry):
        for copy in one_copies(c):
            copy.wait()
        return carry

    lax.fori_loop(0, count, wait_one, 0)

    eye = (
        lax.broadcasted_iota(jnp.int32, (orbitals, orbitals), 0)
        == lax.broadcasted_iota(jnp.int32, (orbitals, orbitals), 1)
    ).astype(BF16)
    my_rows = pl.ds(pl.multiple_of(q * share, share), share)

    def mix_copies(c):
        copies = []
        for e in range(1, wide):
            to = lax.rem(q + e, wide)
            copies.append(
                send(
                    mix.at[c, pl.ds(pl.multiple_of(to * share, share), share)],
                    row_mix.at[q, c],
                    mix_s.at[e - 1, c],
                    mix_r.at[e - 1, c],
                    s,
                    to,
                )
            )
        return copies

    def term_two(c, carry):
        right = jnp.concatenate([one_t[slot_ref[c, k]] for k in range(slots)], axis=0)
        term = jnp.dot(scaled[c], right, preferred_element_type=F32)
        probe = lax.dot_general(
            eye, near[count + c], (((1,), (1,)), ((), ())), preferred_element_type=F32
        )
        second = 2.0 * term - probe
        mix[c] = (COEFF_ZERO * probe + COEFF_ONE * first[c] + COEFF_TWO * second).astype(BF16)
        row_mix[q, c] = mix[c, my_rows, :]
        for copy in mix_copies(c):
            copy.start()
        return carry

    lax.fori_loop(0, count, term_two, 0)

    def product(w, t):
        left = row_mix[lax.rem(q + wide - w, wide)].reshape(count * share, span)
        source = near if w == 0 else rest.at[w - 1]
        right = jnp.concatenate([source[2 * t], source[2 * t + 1]], axis=1)
        part = jnp.dot(left, right, preferred_element_type=F32)
        return [
            part[:, h * orbitals : (h + 1) * orbitals].reshape(count, share, orbitals)
            for h in range(2)
        ]

    def overlap_own(t, carry):
        dense[2 * t], dense[2 * t + 1] = product(0, t)
        return carry

    lax.fori_loop(0, 3 * count // 2, overlap_own, 0)

    for copy in fwd_out + chip_out:
        copy.wait_recv()

    def wait_mix(c, carry):
        for copy in mix_copies(c):
            copy.wait()
        return carry

    lax.fori_loop(0, count, wait_mix, 0)

    def overlap_rest(t, carry):
        for w in range(1, wide):
            low, high = product(w, t)
            dense[2 * t] = dense[2 * t] + low
            dense[2 * t + 1] = dense[2 * t + 1] + high
        return carry

    lax.fori_loop(0, 3 * count // 2, overlap_rest, 0)

    padded = col_force.shape[1]

    def forces(c, carry):
        acc = [jnp.zeros((share, orbitals), F32) for _ in range(3)]
        for k in range(slots):
            sample = dense[slot_ref[c, k], c]
            for m in range(3):
                value = sample * slope[c, k, m]
                acc[m] = acc[m] + value
                col_force[c, k, m] = jnp.sum(
                    value.reshape(share // 8, 8, orbitals), axis=0
                )
        for m in range(3):
            row_force[m, c] = jnp.sum(acc[m].reshape(turns, height, orbitals), axis=0)
        return carry

    for k in range(slots, padded):
        for c in range(count):
            for m in range(3):
                col_force[c, k, m] = jnp.zeros((8, orbitals), F32)
    lax.fori_loop(0, count, forces, 0)

    ids = lax.broadcasted_iota(jnp.int32, (3 * count, slots), 0)
    held_ids = jnp.where(
        ids < count,
        ids + down * count,
        jnp.where(ids < 2 * count, ids - count + s * count, ids - 2 * count + up * count),
    )
    blank = jnp.zeros((3 * count, padded - slots), F32)
    picked = jnp.concatenate(
        [
            part
            for c in range(count)
            for part in (
                jnp.where(wanted_ref[c : c + 1, :] == held_ids, 1.0, 0.0),
                blank,
            )
        ],
        axis=1,
    )
    for m in range(3):
        column = jnp.sum(
            col_force[:, :, m].reshape(count * padded, 8, orbitals), axis=1
        )
        moved = jnp.dot(
            picked, column, precision=lax.Precision.HIGHEST, preferred_element_type=F32
        )
        pull[m] = fold(moved)
        line = jnp.sum(row_force[m], axis=2, keepdims=True) * hit
        pull[m, own] = pull[m, own] - jnp.sum(line, axis=1)
    arrived[1, q] = pull[:, own]
    pull_out = []
    for e in range(wide):
        to = lax.rem(q + e, wide)
        moves = [(pull.at[:, after], 0, up), (pull.at[:, before], 2, down)]
        if e > 0:
            moves.append((pull.at[:, own], 1, s))
        for src, kind, to_space in moves:
            copy = send(
                src, arrived.at[kind, q], pull_s.at[kind, e], pull_r.at[kind, e], to_space, to
            )
            copy.start()
            pull_out.append(copy)

    def density(k, carry):
        for c in range(count):
            sample = dense[slot_ref[c, k], c] * (alive_ref[c, k] * scale)
            stage[pl.ds(c, share, stride=count), :] = sample
        dens_ref[:, k] = stage[...].reshape(share, count, orbitals).astype(dens_ref.dtype)
        return carry

    lax.fori_loop(0, slots, density, 0)
    for copy in pull_out:
        copy.wait()
    result = None
    for kind in range(3):
        for w in range(wide):
            part = arrived[kind, w]
            result = part if result is None else result + part
    force_ref[...] = (result * (-1.0 / total))[:, :, :atoms]

    for copy in [pos_up, pos_down, probe_up, probe_down] + own_out + fwd_out + chip_out:
        copy.wait_send()


def per_device(positions, probes, neighbours):
    count, _, atoms = positions.shape
    slots = neighbours.shape[1]
    orbitals = 4 * atoms
    span = probes.shape[1]
    space = lax.axis_size("space")
    wide = lax.axis_size("probe")
    share = orbitals // wide
    sizes = (space, wide, count, atoms, slots, span, share)
    vmem = pl.BlockSpec(memory_space=pltpu.VMEM)
    dma = pltpu.SemaphoreType.DMA
    peers = max(wide - 1, 1)
    steps = space.bit_length() - 1
    density, force = pl.pallas_call(
        functools.partial(kernel, sizes),
        name="band_forces",
        out_shape=(
            jax.ShapeDtypeStruct((share, slots, count, orbitals), BF16),
            jax.ShapeDtypeStruct((3, count, atoms), F32),
        ),
        in_specs=[pl.BlockSpec(memory_space=pl.ANY)] * 3,
        out_specs=(vmem, vmem),
        scratch_shapes=[
            pltpu.SMEM((count, slots), jnp.int32),
            pltpu.SMEM((count, slots), jnp.int32),
            pltpu.SMEM((count, slots), F32),
            pltpu.VMEM((count, slots), jnp.int32),
            pltpu.VMEM((3, 3, count, atoms), BF16),
            pltpu.VMEM((count, 3, atoms, orbitals), F32),
            pltpu.VMEM((3 * count, span, orbitals), BF16),
            pltpu.VMEM((peers, 3 * count, span, orbitals), BF16),
            pltpu.VMEM((3, 3 * count, orbitals), F32),
            pltpu.VMEM((count, orbitals, slots * orbitals), F32),
            pltpu.VMEM((count, orbitals, slots * orbitals), BF16),
            pltpu.VMEM((count, slots, 7, atoms, orbitals), F32),
            pltpu.VMEM((steps, 8, LANES), F32),
            pltpu.VMEM((steps, 8, LANES), F32),
            pltpu.VMEM((count, slots, 3, share, orbitals), F32),
            pltpu.VMEM((count, orbitals, span), F32),
            pltpu.VMEM((3 * count, orbitals, span), BF16),
            pltpu.VMEM((count, orbitals, span), BF16),
            pltpu.VMEM((wide, count, share, span), BF16),
            pltpu.VMEM((3 * count, count, share, orbitals), F32),
            pltpu.VMEM((share * count, orbitals), F32),
            pltpu.VMEM((count, -(-slots // 8) * 8, 3, 8, orbitals), F32),
            pltpu.VMEM((3, count, min(atoms, share), orbitals), F32),
            pltpu.VMEM((3, 3 * count, orbitals), F32),
            pltpu.VMEM((3, wide, 3, count, orbitals), F32),
            dma((4,)),
            dma((2,)),
            dma((2,)),
            dma((2,)),
            dma((2,)),
            dma((peers,)),
            dma((peers,)),
            dma((peers,)),
            dma((peers,)),
            dma((peers,)),
            dma((peers,)),
            dma((steps,)),
            dma((steps,)),
            dma((2, count)),
            dma((2, count)),
            dma((peers, count)),
            dma((peers, count)),
            dma((3, wide)),
            dma((3, wide)),
        ],
        compiler_params=pltpu.CompilerParams(
            collective_id=0, has_side_effects=True, vmem_limit_bytes=60 * 1024 * 1024
        ),
    )(neighbours, jnp.transpose(positions, (1, 0, 2)), probes)
    return jnp.transpose(density, (0, 2, 1, 3)), jnp.transpose(force, (1, 0, 2))


def solution(mesh):
    in_specs = (P("space", None, None), P("space", "probe", None), P("space", None))
    out_specs = (P("probe", "space", None, None), P("space", None, None))
    return jax.shard_map(
        per_device, mesh=mesh, in_specs=in_specs, out_specs=out_specs, check_vma=False
    )
```

```python
import functools

import jax
import jax.numpy as jnp
from jax import lax
from jax.experimental import pallas as pl
from jax.experimental.pallas import tpu as pltpu
from jax.sharding import PartitionSpec as P

SS_SIGMA = -1.938
SP_SIGMA = 1.745
PP_SIGMA = 3.05
PP_PI = -1.075
PP_DIFF = PP_SIGMA - PP_PI
BOND_LENGTH = 2.35
SOFT_SQUARE = 0.25
CELL_EDGE = 10.86
COEFF_ZERO = 0.6
COEFF_ONE = -0.7
COEFF_TWO = 0.45
MESH = pl.DeviceIdType.MESH
LANES = 128
F32 = jnp.float32
BF16 = jnp.bfloat16


def offsets():
    half = CELL_EDGE / 2.0
    table = [(0.0, 0.0, 0.0)]
    for x in (-1.0, 1.0):
        for y in (-1.0, 1.0):
            for z in (-1.0, 1.0):
                table.append((x * half, y * half, z * half))
    for axis in range(3):
        for sign in (1.0, -1.0):
            entry = [0.0, 0.0, 0.0]
            entry[axis] = sign * CELL_EDGE
            table.append(tuple(entry))
    return table


SHIFTS = offsets()
PIECES = 8


def kernel(
    sizes,
    neighbours_ref,
    positions_ref,
    probes_ref,
    dens_ref,
    force_ref,
    names_ref,
    slot_ref,
    alive_ref,
    wanted_ref,
    raw_pos,
    posc_ref,
    near,
    rest,
    near_pos,
    ham,
    scaled,
    pair,
    top_out,
    top_in,
    slope,
    first,
    one_t,
    mix,
    row_mix,
    dense,
    stage,
    col_force,
    row_force,
    pull,
    arrived,
    local_sem,
    pos_s,
    pos_r,
    probe_s,
    probe_r,
    own_s,
    own_r,
    fwd_s,
    fwd_r,
    chip_s,
    chip_r,
    max_s,
    max_r,
    one_s,
    one_r,
    mix_s,
    mix_r,
    pull_s,
    pull_r,
):
    space, wide, count, atoms, slots, span, share = sizes
    orbitals = 4 * atoms
    total = span * wide
    s = lax.axis_index("space")
    q = lax.axis_index("probe")
    up = lax.rem(s + 1, space)
    down = lax.rem(s + space - 1, space)
    before, own, after = pl.ds(0, count), pl.ds(count, count), pl.ds(2 * count, count)
    core = lax.rem(s, 2)
    mate = s + 1 - 2 * core
    far_side = pl.ds(core * (2 * count), count)

    def send(src, dst, ss, rs, to_space, to_probe):
        return pltpu.make_async_remote_copy(
            src_ref=src,
            dst_ref=dst,
            send_sem=ss,
            recv_sem=rs,
            device_id={"space": to_space, "probe": to_probe},
            device_id_type=MESH,
        )

    steps = space.bit_length() - 1
    partners = []
    for j in range(steps):
        bit = lax.rem(lax.div(s, 2**j), 2)
        partners.append(s + 2**j * (1 - 2 * bit))

    barrier = pltpu.get_barrier_semaphore()

    def greet(to_space, to_probe):
        pl.semaphore_signal(
            barrier,
            inc=1,
            device_id={"space": to_space, "probe": to_probe},
            device_id_type=MESH,
        )

    for to in partners + [up, down]:
        greet(to, q)
    for e in range(1, wide):
        for to in (s, up, down):
            greet(to, lax.rem(q + e, wide))

    loads = [
        pltpu.make_async_copy(src, dst, local_sem.at[i])
        for i, (src, dst) in enumerate(
            [
                (positions_ref, raw_pos.at[1]),
                (neighbours_ref, names_ref),
                (neighbours_ref, wanted_ref),
                (probes_ref, near.at[own]),
            ]
        )
    ]
    for load in loads:
        load.start()
    pl.semaphore_wait(barrier, steps + 2 + 3 * (wide - 1))

    pos_up = send(positions_ref, raw_pos.at[0], pos_s.at[0], pos_r.at[0], up, q)
    pos_down = send(positions_ref, raw_pos.at[2], pos_s.at[1], pos_r.at[1], down, q)
    pos_up.start()
    pos_down.start()
    probe_up = send(probes_ref, near.at[before], probe_s.at[0], probe_r.at[0], up, q)
    probe_down = send(probes_ref, near.at[after], probe_s.at[1], probe_r.at[1], down, q)
    probe_up.start()
    probe_down.start()
    own_out = []
    for e in range(1, wide):
        copy = send(
            probes_ref,
            rest.at[e - 1, own],
            own_s.at[e - 1],
            own_r.at[e - 1],
            s,
            lax.rem(q + e, wide),
        )
        copy.start()
        own_out.append(copy)

    def fold(x):
        return (
            x
            + pltpu.roll(x, atoms, 1)
            + pltpu.roll(x, 2 * atoms, 1)
            + pltpu.roll(x, 3 * atoms, 1)
        )

    def spread(part):
        rows = pl.ds(part * count, count)
        for m in range(3):
            near_pos[m, rows, :atoms] = raw_pos[part, m].astype(F32)
            near_pos[m, rows] = fold(jnp.where(narrow, near_pos[m, rows], 0.0))

    for load in loads[:3]:
        load.wait()
    narrow = lax.broadcasted_iota(jnp.int32, (count, orbitals), 1) < atoms
    spread(1)
    for m in range(3):
        tall = jnp.transpose(near_pos[m, own])
        for c in range(count):
            posc_ref[c, m] = jnp.broadcast_to(tall[:atoms, c : c + 1], (atoms, orbitals))

    def find_slots(c, carry):
        for k in range(slots):
            name = names_ref[c, k]
            held = jnp.maximum(name, 0)
            place = lax.rem(lax.div(held, count) - s + 1 + space, space) * count
            place = place + lax.rem(held, count)
            slot_ref[c, k] = jnp.where(name >= 0, jnp.minimum(place, 3 * count - 1), count)
            alive_ref[c, k] = jnp.where(name >= 0, 1.0, 0.0)
        return carry

    lax.fori_loop(0, count, find_slots, 0)
    pos_up.wait_recv()
    spread(0)
    pos_down.wait_recv()
    spread(2)

    lane = lax.broadcasted_iota(jnp.int32, (atoms, orbitals), 1)
    group = lane // atoms
    is_s = group == 0
    is_p = [group == 1, group == 2, group == 3]
    pp = [jnp.where(m, PP_PI, 0.0).astype(F32) for m in is_p]

    def peak_of(c, peak):
        rows = [posc_ref[c, m] for m in range(3)]
        sums = [jnp.zeros((atoms, orbitals), F32) for _ in range(4)]
        for k in range(0, slots, 4):
            picked = range(k, min(k + 4, slots))
            alive = jnp.zeros((1, orbitals), F32)
            column = [jnp.zeros((1, orbitals), F32) for _ in range(3)]
            for i, t in enumerate(picked):
                here = group[:1] == i
                alive = jnp.where(here, alive_ref[c, t], alive)
                place = slot_ref[c, t]
                for m in range(3):
                    column[m] = jnp.where(
                        here, near_pos[m, pl.ds(place, 1), :] + SHIFTS[t][m], column[m]
                    )
            d = [column[m] - rows[m] for m in range(3)]
            square = d[0] * d[0] + d[1] * d[1] + d[2] * d[2] + SOFT_SQUARE
            inv = lax.rsqrt(square)
            u = [jnp.abs(x) * inv for x in d]
            g = jnp.exp(1.0 - square * (1.0 / (BOND_LENGTH * BOND_LENGTH))) * alive
            sums[0] = sums[0] + g * ((u[0] + u[1] + u[2]) * SP_SIGMA - SS_SIGMA)
            for a in range(3):
                others = u[(a + 1) % 3] + u[(a + 2) % 3]
                value = u[a] * (others * PP_DIFF + SP_SIGMA)
                value = value + jnp.abs(u[a] * u[a] * PP_DIFF + PP_PI)
                sums[1 + a] = sums[1 + a] + g * value
        for a in range(4):
            peak = jnp.maximum(peak, jnp.sum(sums[a], axis=1, keepdims=True))
        return peak

    def build(c, carry):
        rows = [posc_ref[c, m] for m in range(3)]
        for k in range(slots):
            place = slot_ref[c, k]
            alive = alive_ref[c, k]
            d = [
                (near_pos[m, pl.ds(place, 1), :] + SHIFTS[k][m]) - rows[m] for m in range(3)
            ]
            square = d[0] * d[0] + d[1] * d[1] + d[2] * d[2] + SOFT_SQUARE
            inv = lax.rsqrt(square)
            l = [x * inv for x in d]
            g = jnp.exp(1.0 - square * (1.0 / (BOND_LENGTH * BOND_LENGTH))) * alive
            beta = jnp.where(
                is_s, 0.0, jnp.where(is_p[0], l[0], jnp.where(is_p[1], l[1], l[2]))
            )
            coef_s = jnp.where(is_s, SS_SIGMA, SP_SIGMA * beta)
            coef_p = jnp.where(is_s, -SP_SIGMA, PP_DIFF * beta)
            parts = [coef_s * g] + [(l[m] * coef_p + pp[m]) * g for m in range(3)]
            for a in range(4):
                ham[c, a * atoms : (a + 1) * atoms, k * orbitals : (k + 1) * orbitals] = parts[a]
            pair[c, k, 0] = jnp.zeros_like(g)
            for m in range(3):
                pair[c, k, 1 + m] = l[m]
            pair[c, k, 4] = beta
            pair[c, k, 5] = g * inv
            pair[c, k, 6] = g * (square * inv) * (2.0 / (BOND_LENGTH * BOND_LENGTH))
        return carry

    peak = lax.fori_loop(0, count, peak_of, jnp.zeros((atoms, 1), F32))
    top = jnp.broadcast_to(jnp.max(peak, axis=0, keepdims=True), (8, LANES))
    order = [0] + list(range(2, steps)) + ([1] if steps > 1 else [])
    done = 0
    for t, j in enumerate(order):
        top_out[j] = top
        copy = send(top_out.at[j], top_in.at[j], max_s.at[j], max_r.at[j], partners[j], q)
        copy.start()
        until = count if t == len(order) - 1 else count * (t + 1) // len(order)
        lax.fori_loop(done, until, build, 0)
        done = until
        copy.wait()
        top = jnp.maximum(top, top_in[j])
    shrink = 1.0 / top[0:1]

    loads[3].wait()
    probe_up.wait_recv()
    probe_down.wait_recv()
    fwd_out = []
    for e in range(1, wide):
        copy = send(
            near.at[far_side],
            rest.at[e - 1, far_side],
            fwd_s.at[e - 1],
            fwd_r.at[e - 1],
            s,
            lax.rem(q + e, wide),
        )
        copy.start()
        fwd_out.append(copy)

    def one_copies(c):
        return (
            send(one_t.at[count + c], one_t.at[c], one_s.at[0, c], one_r.at[0, c], up, q),
            send(
                one_t.at[count + c], one_t.at[2 * count + c], one_s.at[1, c], one_r.at[1, c], down, q
            ),
        )

    def term_one(c, carry):
        for k in range(slots):
            part = pl.ds(k * orbitals, orbitals)
            scaled[c, :, part] = (ham[c, :, part] * shrink).astype(BF16)
        right = jnp.concatenate([near[slot_ref[c, k]] for k in range(slots)], axis=1)
        term = lax.dot_general(
            scaled[c], right, (((1,), (1,)), ((), ())), preferred_element_type=F32
        )
        first[c] = term
        one_t[count + c] = term.astype(BF16)
        for copy in one_copies(c):
            copy.start()
        return carry

    lax.fori_loop(0, count, term_one, 0)

    chip_out = []
    for e in range(1, wide):
        own_out[e - 1].wait_recv()
        copy = send(
            rest.at[e - 1, own],
            rest.at[e - 1, far_side],
            chip_s.at[e - 1],
            chip_r.at[e - 1],
            mate,
            q,
        )
        copy.start()
        chip_out.append(copy)

    height = min(atoms, share)
    turns = share // height
    start_atom = lax.rem(q * share, atoms)
    rows = pl.ds(pl.multiple_of(start_atom, height), height)
    s_mask = jnp.where(is_s[:height], 1.0, 0.0).astype(F32)
    p_mask = [jnp.where(m[:height], 1.0, 0.0).astype(F32) for m in is_p]
    row_iota = lax.broadcasted_iota(jnp.int32, (height, orbitals), 0) + start_atom
    hit = jnp.where(row_iota == lax.rem(lane[:height], atoms), 1.0, 0.0).astype(F32)
    scale = 1.0 / float(total) ** 0.5

    def slopes(c, carry):
        for t in range(turns):
            kind = (q * share) // atoms + t
            ws = jnp.where(kind == 0, 1.0, 0.0).astype(F32)
            wr = [jnp.where(kind == m + 1, 1.0, 0.0).astype(F32) for m in range(3)]
            wv = PP_PI * (wr[0] * p_mask[0] + wr[1] * p_mask[1] + wr[2] * p_mask[2])
            wv = wv + (ws * SS_SIGMA) * s_mask
            for k in range(slots):
                alpha = pair[c, k, kind, rows, :]
                beta = pair[c, k, 4, rows, :]
                lean = pair[c, k, 5, rows, :]
                c_one = PP_DIFF * alpha + ws * SP_SIGMA
                c_two = PP_DIFF * beta - SP_SIGMA * s_mask
                cross = alpha * c_two
                bracket = (ws * SP_SIGMA) * beta + cross + wv
                x = lean * c_one
                y = lean * c_two
                drag = lean * (c_one * beta + cross) + pair[c, k, 6, rows, :] * bracket
                for m in range(3):
                    slope[c, k, m, t * height : (t + 1) * height] = (
                        x * p_mask[m] + y * wr[m] - drag * pair[c, k, 1 + m, rows, :]
                    )
        return carry

    lax.fori_loop(0, count, slopes, 0)

    def wait_one(c, carry):
        for copy in one_copies(c):
            copy.wait()
        return carry

    lax.fori_loop(0, count, wait_one, 0)

    eye = (
        lax.broadcasted_iota(jnp.int32, (orbitals, orbitals), 0)
        == lax.broadcasted_iota(jnp.int32, (orbitals, orbitals), 1)
    ).astype(BF16)
    my_rows = pl.ds(pl.multiple_of(q * share, share), share)

    def mix_copies(c):
        copies = []
        for e in range(1, wide):
            to = lax.rem(q + e, wide)
            copies.append(
                send(
                    mix.at[c, pl.ds(pl.multiple_of(to * share, share), share)],
                    row_mix.at[q, c],
                    mix_s.at[e - 1, c],
                    mix_r.at[e - 1, c],
                    s,
                    to,
                )
            )
        return copies

    def term_two(c, carry):
        right = jnp.concatenate([one_t[slot_ref[c, k]] for k in range(slots)], axis=0)
        term = jnp.dot(scaled[c], right, preferred_element_type=F32)
        probe = lax.dot_general(
            eye, near[count + c], (((1,), (1,)), ((), ())), preferred_element_type=F32
        )
        second = 2.0 * term - probe
        mix[c] = (COEFF_ZERO * probe + COEFF_ONE * first[c] + COEFF_TWO * second).astype(BF16)
        row_mix[q, c] = mix[c, my_rows, :]
        for copy in mix_copies(c):
            copy.start()
        return carry

    lax.fori_loop(0, count, term_two, 0)

    def product(w, t):
        left = row_mix[lax.rem(q + wide - w, wide)].reshape(count * share, span)
        source = near if w == 0 else rest.at[w - 1]
        right = jnp.concatenate([source[2 * t], source[2 * t + 1]], axis=1)
        part = jnp.dot(left, right, preferred_element_type=F32)
        return [
            part[:, h * orbitals : (h + 1) * orbitals].reshape(count, share, orbitals)
            for h in range(2)
        ]

    def overlap_own(t, carry):
        dense[2 * t], dense[2 * t + 1] = product(0, t)
        return carry

    lax.fori_loop(0, 3 * count // 2, overlap_own, 0)

    for copy in fwd_out + chip_out:
        copy.wait_recv()

    def wait_mix(c, carry):
        for copy in mix_copies(c):
            copy.wait()
        return carry

    lax.fori_loop(0, count, wait_mix, 0)

    def overlap_rest(t, carry):
        for w in range(1, wide):
            low, high = product(w, t)
            dense[2 * t] = dense[2 * t] + low
            dense[2 * t + 1] = dense[2 * t + 1] + high
        return carry

    lax.fori_loop(0, 3 * count // 2, overlap_rest, 0)

    padded = col_force.shape[1]

    def forces(c, carry):
        acc = [jnp.zeros((share, orbitals), F32) for _ in range(3)]
        for k in range(slots):
            sample = dense[slot_ref[c, k], c]
            for m in range(3):
                value = sample * slope[c, k, m]
                acc[m] = acc[m] + value
                col_force[c, k, m] = jnp.sum(
                    value.reshape(share // 8, 8, orbitals), axis=0
                )
        for m in range(3):
            row_force[m, c] = jnp.sum(acc[m].reshape(turns, height, orbitals), axis=0)
        return carry

    for k in range(slots, padded):
        for c in range(count):
            for m in range(3):
                col_force[c, k, m] = jnp.zeros((8, orbitals), F32)
    lax.fori_loop(0, count, forces, 0)

    ids = lax.broadcasted_iota(jnp.int32, (3 * count, slots), 0)
    held_ids = jnp.where(
        ids < count,
        ids + down * count,
        jnp.where(ids < 2 * count, ids - count + s * count, ids - 2 * count + up * count),
    )
    blank = jnp.zeros((3 * count, padded - slots), F32)
    picked = jnp.concatenate(
        [
            part
            for c in range(count)
            for part in (
                jnp.where(wanted_ref[c : c + 1, :] == held_ids, 1.0, 0.0),
                blank,
            )
        ],
        axis=1,
    )
    for m in range(3):
        column = jnp.sum(
            col_force[:, :, m].reshape(count * padded, 8, orbitals), axis=1
        )
        moved = jnp.dot(
            picked, column, precision=lax.Precision.HIGHEST, preferred_element_type=F32
        )
        pull[m] = fold(moved)
        line = jnp.sum(row_force[m], axis=2, keepdims=True) * hit
        pull[m, own] = pull[m, own] - jnp.sum(line, axis=1)
    arrived[1, q] = pull[:, own]
    pull_out = []
    for e in range(wide):
        to = lax.rem(q + e, wide)
        moves = [(pull.at[:, after], 0, up), (pull.at[:, before], 2, down)]
        if e > 0:
            moves.append((pull.at[:, own], 1, s))
        for src, kind, to_space in moves:
            copy = send(
                src, arrived.at[kind, q], pull_s.at[kind, e], pull_r.at[kind, e], to_space, to
            )
            copy.start()
            pull_out.append(copy)

    def density(k, carry):
        for c in range(count):
            sample = dense[slot_ref[c, k], c] * (alive_ref[c, k] * scale)
            stage[pl.ds(c, share, stride=count), :] = sample
        dens_ref[:, k] = stage[...].reshape(share, count, orbitals).astype(dens_ref.dtype)
        return carry

    lax.fori_loop(0, slots, density, 0)
    for copy in pull_out:
        copy.wait()
    result = None
    for kind in range(3):
        for w in range(wide):
            part = arrived[kind, w]
            result = part if result is None else result + part
    force_ref[...] = (result * (-1.0 / total))[:, :, :atoms]

    for copy in [pos_up, pos_down, probe_up, probe_down] + own_out + fwd_out + chip_out:
        copy.wait_send()


def write_out(pieces, dens_in, force_in, dens_out, force_out, sems):
    rows = dens_in.shape[0] // pieces
    copies = [pltpu.make_async_copy(force_in, force_out, sems.at[pieces])]
    for i in range(pieces):
        part = pl.ds(i * rows, rows)
        copies.append(pltpu.make_async_copy(dens_in.at[part], dens_out.at[part], sems.at[i]))
    for copy in copies:
        copy.start()
    for copy in copies:
        copy.wait()


def per_device(positions, probes, neighbours):
    count, _, atoms = positions.shape
    slots = neighbours.shape[1]
    orbitals = 4 * atoms
    span = probes.shape[1]
    space = lax.axis_size("space")
    wide = lax.axis_size("probe")
    share = orbitals // wide
    sizes = (space, wide, count, atoms, slots, span, share)
    vmem = pl.BlockSpec(memory_space=pltpu.VMEM)
    dma = pltpu.SemaphoreType.DMA
    peers = max(wide - 1, 1)
    steps = space.bit_length() - 1
    density, force = pl.pallas_call(
        functools.partial(kernel, sizes),
        name="band_forces",
        out_shape=(
            pltpu.VMEM((share, slots, count, orbitals), BF16),
            pltpu.VMEM((3, count, atoms), F32),
        ),
        in_specs=[pl.BlockSpec(memory_space=pl.ANY)] * 3,
        out_specs=(vmem, vmem),
        scratch_shapes=[
            pltpu.SMEM((count, slots), jnp.int32),
            pltpu.SMEM((count, slots), jnp.int32),
            pltpu.SMEM((count, slots), F32),
            pltpu.VMEM((count, slots), jnp.int32),
            pltpu.VMEM((3, 3, count, atoms), BF16),
            pltpu.VMEM((count, 3, atoms, orbitals), F32),
            pltpu.VMEM((3 * count, span, orbitals), BF16),
            pltpu.VMEM((peers, 3 * count, span, orbitals), BF16),
            pltpu.VMEM((3, 3 * count, orbitals), F32),
            pltpu.VMEM((count, orbitals, slots * orbitals), F32),
            pltpu.VMEM((count, orbitals, slots * orbitals), BF16),
            pltpu.VMEM((count, slots, 7, atoms, orbitals), F32),
            pltpu.VMEM((steps, 8, LANES), F32),
            pltpu.VMEM((steps, 8, LANES), F32),
            pltpu.VMEM((count, slots, 3, share, orbitals), F32),
            pltpu.VMEM((count, orbitals, span), F32),
            pltpu.VMEM((3 * count, orbitals, span), BF16),
            pltpu.VMEM((count, orbitals, span), BF16),
            pltpu.VMEM((wide, count, share, span), BF16),
            pltpu.VMEM((3 * count, count, share, orbitals), F32),
            pltpu.VMEM((share * count, orbitals), F32),
            pltpu.VMEM((count, -(-slots // 8) * 8, 3, 8, orbitals), F32),
            pltpu.VMEM((3, count, min(atoms, share), orbitals), F32),
            pltpu.VMEM((3, 3 * count, orbitals), F32),
            pltpu.VMEM((3, wide, 3, count, orbitals), F32),
            dma((4,)),
            dma((2,)),
            dma((2,)),
            dma((2,)),
            dma((2,)),
            dma((peers,)),
            dma((peers,)),
            dma((peers,)),
            dma((peers,)),
            dma((peers,)),
            dma((peers,)),
            dma((steps,)),
            dma((steps,)),
            dma((2, count)),
            dma((2, count)),
            dma((peers, count)),
            dma((peers, count)),
            dma((3, wide)),
            dma((3, wide)),
        ],
        compiler_params=pltpu.CompilerParams(
            collective_id=0, has_side_effects=True, vmem_limit_bytes=60 * 1024 * 1024
        ),
    )(neighbours, jnp.transpose(positions, (1, 0, 2)), probes)
    anywhere = pl.BlockSpec(memory_space=pl.ANY)
    density, force = pl.pallas_call(
        functools.partial(write_out, PIECES),
        name="write_out",
        out_shape=(
            jax.ShapeDtypeStruct(density.shape, BF16),
            jax.ShapeDtypeStruct(force.shape, F32),
        ),
        in_specs=[vmem, vmem],
        out_specs=(anywhere, anywhere),
        scratch_shapes=[dma((PIECES + 1,))],
        compiler_params=pltpu.CompilerParams(vmem_limit_bytes=1024 * 1024),
    )(density, force)
    return jnp.transpose(density, (0, 2, 1, 3)), jnp.transpose(force, (1, 0, 2))


def solution(mesh):
    in_specs = (P("space", None, None), P("space", "probe", None), P("space", None))
    out_specs = (P("probe", "space", None, None), P("space", None, None))
    return jax.shard_map(
        per_device, mesh=mesh, in_specs=in_specs, out_specs=out_specs, check_vma=False
    )
```

```python
import functools

import jax
import jax.numpy as jnp
from jax import lax
from jax.experimental import pallas as pl
from jax.experimental.pallas import tpu as pltpu
from jax.sharding import PartitionSpec as P

SS_SIGMA = -1.938
SP_SIGMA = 1.745
PP_SIGMA = 3.05
PP_PI = -1.075
PP_DIFF = PP_SIGMA - PP_PI
BOND_LENGTH = 2.35
SOFT_SQUARE = 0.25
CELL_EDGE = 10.86
COEFF_ZERO = 0.6
COEFF_ONE = -0.7
COEFF_TWO = 0.45
MESH = pl.DeviceIdType.MESH
LANES = 128
F32 = jnp.float32
BF16 = jnp.bfloat16


def offsets():
    half = CELL_EDGE / 2.0
    table = [(0.0, 0.0, 0.0)]
    for x in (-1.0, 1.0):
        for y in (-1.0, 1.0):
            for z in (-1.0, 1.0):
                table.append((x * half, y * half, z * half))
    for axis in range(3):
        for sign in (1.0, -1.0):
            entry = [0.0, 0.0, 0.0]
            entry[axis] = sign * CELL_EDGE
            table.append(tuple(entry))
    return table


SHIFTS = offsets()
PIECES = 8
EARLY_BUILD = 3
EARLY_SLOPES = 2


def kernel(
    sizes,
    neighbours_ref,
    positions_ref,
    probes_ref,
    dens_ref,
    force_ref,
    names_ref,
    slot_ref,
    alive_ref,
    wanted_ref,
    raw_pos,
    posc_ref,
    near,
    rest,
    near_pos,
    ham,
    scaled,
    pair,
    top_out,
    top_in,
    slope,
    first,
    one_t,
    mix,
    row_mix,
    dense,
    stage,
    col_force,
    row_force,
    pull,
    arrived,
    local_sem,
    pos_s,
    pos_r,
    probe_s,
    probe_r,
    own_s,
    own_r,
    fwd_s,
    fwd_r,
    chip_s,
    chip_r,
    max_s,
    max_r,
    one_s,
    one_r,
    mix_s,
    mix_r,
    pull_s,
    pull_r,
):
    space, wide, count, atoms, slots, span, share, chunks, plane = sizes
    width = span // chunks
    orbitals = 4 * atoms
    total = span * wide
    s = lax.axis_index("space")
    q = lax.axis_index("probe")
    up = lax.rem(s + 1, space)
    down = lax.rem(s + space - 1, space)
    before, own, after = pl.ds(0, count), pl.ds(count, count), pl.ds(2 * count, count)
    core = lax.rem(s, 2)
    mate = s + 1 - 2 * core
    far_side = pl.ds(core * (2 * count), count)

    def send(src, dst, ss, rs, to_space, to_probe):
        return pltpu.make_async_remote_copy(
            src_ref=src,
            dst_ref=dst,
            send_sem=ss,
            recv_sem=rs,
            device_id={"space": to_space, "probe": to_probe},
            device_id_type=MESH,
        )

    low, high = lax.rem(s, plane), lax.div(s, plane)
    planes = space // plane
    beside = [high * plane + lax.rem(low + d, plane) for d in range(1, plane)]
    across = [lax.rem(high + d, planes) * plane + low for d in range(1, planes)]

    barrier = pltpu.get_barrier_semaphore()

    def greet(to_space, to_probe):
        pl.semaphore_signal(
            barrier,
            inc=1,
            device_id={"space": to_space, "probe": to_probe},
            device_id_type=MESH,
        )

    for to in beside + across + [up, down]:
        greet(to, q)
    for e in range(1, wide):
        for to in (s, up, down):
            greet(to, lax.rem(q + e, wide))

    loads = [
        pltpu.make_async_copy(src, dst, local_sem.at[i])
        for i, (src, dst) in enumerate(
            [
                (positions_ref, raw_pos.at[1]),
                (neighbours_ref, names_ref),
                (neighbours_ref, wanted_ref),
            ]
            + [
                (probes_ref.at[:, pl.ds(j * width, width)], near[j].at[own])
                for j in range(chunks)
            ]
        )
    ]
    for load in loads:
        load.start()
    pl.semaphore_wait(barrier, plane + planes + 3 * (wide - 1))

    pos_up = send(positions_ref, raw_pos.at[0], pos_s.at[0], pos_r.at[0], up, q)
    pos_down = send(positions_ref, raw_pos.at[2], pos_s.at[1], pos_r.at[1], down, q)
    pos_up.start()
    pos_down.start()
    def probe_copies(j):
        part = pl.ds(j * width, width)
        return [
            send(
                probes_ref.at[:, part],
                near[j].at[place],
                probe_s.at[i, j],
                probe_r.at[i, j],
                to,
                q,
            )
            for i, (place, to) in enumerate([(before, up), (after, down)])
        ]

    crossing = jnp.logical_or(lax.rem(s, 4) == 0, lax.rem(s, 4) == 3)

    def start_probes(j, when):
        @pl.when(when)
        def _():
            for copy in probe_copies(j):
                copy.start()

    start_probes(0, jnp.logical_not(crossing))
    def own_copies(j):
        return [
            send(
                probes_ref.at[:, pl.ds(j * width, width)],
                rest[j].at[e - 1, own],
                own_s.at[e - 1, j],
                own_r.at[e - 1, j],
                s,
                lax.rem(q + e, wide),
            )
            for e in range(1, wide)
        ]

    for j in range(chunks):
        for copy in own_copies(j):
            copy.start()

    def fold(x):
        return (
            x
            + pltpu.roll(x, atoms, 1)
            + pltpu.roll(x, 2 * atoms, 1)
            + pltpu.roll(x, 3 * atoms, 1)
        )

    def spread(part):
        rows = pl.ds(part * count, count)
        for m in range(3):
            near_pos[m, rows, :atoms] = raw_pos[part, m].astype(F32)
            near_pos[m, rows] = fold(jnp.where(narrow, near_pos[m, rows], 0.0))

    for load in loads[:3]:
        load.wait()
    narrow = lax.broadcasted_iota(jnp.int32, (count, orbitals), 1) < atoms
    spread(1)
    for m in range(3):
        tall = jnp.transpose(near_pos[m, own])
        for c in range(count):
            posc_ref[c, m] = jnp.broadcast_to(tall[:atoms, c : c + 1], (atoms, orbitals))

    def find_slots(c, carry):
        for k in range(slots):
            name = names_ref[c, k]
            held = jnp.maximum(name, 0)
            place = lax.rem(lax.div(held, count) - s + 1 + space, space) * count
            place = place + lax.rem(held, count)
            slot_ref[c, k] = jnp.where(name >= 0, jnp.minimum(place, 3 * count - 1), count)
            alive_ref[c, k] = jnp.where(name >= 0, 1.0, 0.0)
        return carry

    lax.fori_loop(0, count, find_slots, 0)
    start_probes(0, crossing)
    pos_up.wait_recv()
    spread(0)
    pos_down.wait_recv()
    spread(2)

    lane = lax.broadcasted_iota(jnp.int32, (atoms, orbitals), 1)
    group = lane // atoms
    is_s = group == 0
    is_p = [group == 1, group == 2, group == 3]
    pp = [jnp.where(m, PP_PI, 0.0).astype(F32) for m in is_p]

    def peak_of(c, peak):
        rows = [posc_ref[c, m] for m in range(3)]
        sums = [jnp.zeros((atoms, orbitals), F32) for _ in range(4)]
        for k in range(0, slots, 4):
            picked = range(k, min(k + 4, slots))
            alive = jnp.zeros((1, orbitals), F32)
            column = [jnp.zeros((1, orbitals), F32) for _ in range(3)]
            for i, t in enumerate(picked):
                here = group[:1] == i
                alive = jnp.where(here, alive_ref[c, t], alive)
                place = slot_ref[c, t]
                for m in range(3):
                    column[m] = jnp.where(
                        here, near_pos[m, pl.ds(place, 1), :] + SHIFTS[t][m], column[m]
                    )
            d = [column[m] - rows[m] for m in range(3)]
            square = d[0] * d[0] + d[1] * d[1] + d[2] * d[2] + SOFT_SQUARE
            inv = lax.rsqrt(square)
            u = [jnp.abs(x) * inv for x in d]
            g = jnp.exp(1.0 - square * (1.0 / (BOND_LENGTH * BOND_LENGTH))) * alive
            sums[0] = sums[0] + g * ((u[0] + u[1] + u[2]) * SP_SIGMA - SS_SIGMA)
            for a in range(3):
                others = u[(a + 1) % 3] + u[(a + 2) % 3]
                value = u[a] * (others * PP_DIFF + SP_SIGMA)
                value = value + jnp.abs(u[a] * u[a] * PP_DIFF + PP_PI)
                sums[1 + a] = sums[1 + a] + g * value
        for a in range(4):
            peak = jnp.maximum(peak, jnp.sum(sums[a], axis=1, keepdims=True))
        return peak

    def build(c, carry):
        rows = [posc_ref[c, m] for m in range(3)]
        for k in range(slots):
            place = slot_ref[c, k]
            alive = alive_ref[c, k]
            d = [
                (near_pos[m, pl.ds(place, 1), :] + SHIFTS[k][m]) - rows[m] for m in range(3)
            ]
            square = d[0] * d[0] + d[1] * d[1] + d[2] * d[2] + SOFT_SQUARE
            inv = lax.rsqrt(square)
            l = [x * inv for x in d]
            g = jnp.exp(1.0 - square * (1.0 / (BOND_LENGTH * BOND_LENGTH))) * alive
            beta = jnp.where(
                is_s, 0.0, jnp.where(is_p[0], l[0], jnp.where(is_p[1], l[1], l[2]))
            )
            coef_s = jnp.where(is_s, SS_SIGMA, SP_SIGMA * beta)
            coef_p = jnp.where(is_s, -SP_SIGMA, PP_DIFF * beta)
            parts = [coef_s * g] + [(l[m] * coef_p + pp[m]) * g for m in range(3)]
            for a in range(4):
                ham[c, a * atoms : (a + 1) * atoms, k * orbitals : (k + 1) * orbitals] = parts[a]
            pair[c, k, 0] = jnp.zeros_like(g)
            for m in range(3):
                pair[c, k, 1 + m] = l[m]
            pair[c, k, 4] = beta
            pair[c, k, 5] = g * inv
            pair[c, k, 6] = g * (square * inv) * (2.0 / (BOND_LENGTH * BOND_LENGTH))
        return carry

    height = min(atoms, share)
    turns = share // height
    start_atom = lax.rem(q * share, atoms)
    rows = pl.ds(pl.multiple_of(start_atom, height), height)
    s_mask = jnp.where(is_s[:height], 1.0, 0.0).astype(F32)
    p_mask = [jnp.where(m[:height], 1.0, 0.0).astype(F32) for m in is_p]
    row_iota = lax.broadcasted_iota(jnp.int32, (height, orbitals), 0) + start_atom
    hit = jnp.where(row_iota == lax.rem(lane[:height], atoms), 1.0, 0.0).astype(F32)
    scale = 1.0 / float(total) ** 0.5

    def slopes(c, carry):
        for t in range(turns):
            kind = (q * share) // atoms + t
            ws = jnp.where(kind == 0, 1.0, 0.0).astype(F32)
            wr = [jnp.where(kind == m + 1, 1.0, 0.0).astype(F32) for m in range(3)]
            wv = PP_PI * (wr[0] * p_mask[0] + wr[1] * p_mask[1] + wr[2] * p_mask[2])
            wv = wv + (ws * SS_SIGMA) * s_mask
            for k in range(slots):
                alpha = pair[c, k, kind, rows, :]
                beta = pair[c, k, 4, rows, :]
                lean = pair[c, k, 5, rows, :]
                c_one = PP_DIFF * alpha + ws * SP_SIGMA
                c_two = PP_DIFF * beta - SP_SIGMA * s_mask
                cross = alpha * c_two
                bracket = (ws * SP_SIGMA) * beta + cross + wv
                x = lean * c_one
                y = lean * c_two
                drag = lean * (c_one * beta + cross) + pair[c, k, 6, rows, :] * bracket
                for m in range(3):
                    slope[c, k, m, t * height : (t + 1) * height] = (
                        x * p_mask[m] + y * wr[m] - drag * pair[c, k, 1 + m, rows, :]
                    )
        return carry

    peak = lax.fori_loop(0, count, peak_of, jnp.zeros((atoms, 1), F32))
    top = jnp.broadcast_to(jnp.max(peak, axis=0, keepdims=True), (8, LANES))

    def top_copies(stage, devices):
        base = 0 if stage == 0 else plane - 1
        return [
            send(
                top_out.at[stage],
                top_in.at[base + i],
                max_s.at[base + i],
                max_r.at[base + i],
                to,
                q,
            )
            for i, to in enumerate(devices)
        ]

    def raise_top(top, stage, devices):
        base = 0 if stage == 0 else plane - 1
        for i, copy in enumerate(top_copies(stage, devices)):
            copy.wait()
            top = jnp.maximum(top, top_in[base + i])
        return top

    def forward(j):
        copies = []
        for e in range(1, wide):
            copies.append(
                send(
                    near[j].at[far_side],
                    rest[j].at[e - 1, far_side],
                    fwd_s.at[e - 1, j],
                    fwd_r.at[e - 1, j],
                    s,
                    lax.rem(q + e, wide),
                )
            )
        return copies

    top_out[0] = top
    for copy in top_copies(0, beside):
        copy.start()
    for j in range(1, chunks):
        start_probes(j, jnp.logical_not(crossing))
    lax.fori_loop(0, EARLY_BUILD, build, 0)
    top = raise_top(top, 0, beside)
    top_out[1] = top
    for copy in top_copies(1, across):
        copy.start()
    for j in range(1, chunks):
        start_probes(j, crossing)
    lax.fori_loop(EARLY_BUILD, count, build, 0)
    lax.fori_loop(0, EARLY_SLOPES, slopes, 0)
    for load in loads[3:]:
        load.wait()
    for copy in probe_copies(0):
        copy.wait_recv()
    for copy in forward(0):
        copy.start()
    top = raise_top(top, 1, across)
    shrink = 1.0 / top[0:1]

    def one_copies(j, c):
        return [
            send(
                one_t[j].at[count + c],
                one_t[j].at[place + c],
                one_s.at[i, j, c],
                one_r.at[i, j, c],
                to,
                q,
            )
            for i, (place, to) in enumerate([(0, up), (2 * count, down)])
        ]

    def term_one(j):
        def body(c, carry):
            right = jnp.concatenate([near[j][slot_ref[c, k]] for k in range(slots)], axis=1)
            term = lax.dot_general(
                scaled[c], right, (((1,), (1,)), ((), ())), preferred_element_type=F32
            )
            first[j, c] = term
            one_t[j][count + c] = term.astype(BF16)
            for copy in one_copies(j, c):
                copy.start()
            return carry

        lax.fori_loop(0, count, body, 0)

    def scale_down(c, carry):
        for k in range(slots):
            here = pl.ds(k * orbitals, orbitals)
            scaled[c, :, here] = (ham[c, :, here] * shrink).astype(BF16)
        return carry

    lax.fori_loop(0, count, scale_down, 0)
    term_one(0)
    def later_slopes(when):
        @pl.when(when)
        def _():
            lax.fori_loop(EARLY_SLOPES, count, slopes, 0)

    for j in range(1, chunks):
        for copy in probe_copies(j):
            copy.wait_recv()
        for copy in forward(j):
            copy.start()
    later_slopes(crossing)
    for j in range(1, chunks):
        term_one(j)
    later_slopes(jnp.logical_not(crossing))

    def mate_copies(j):
        return [
            send(
                rest[j].at[e - 1, own],
                rest[j].at[e - 1, far_side],
                chip_s.at[e - 1, j],
                chip_r.at[e - 1, j],
                mate,
                q,
            )
            for e in range(1, wide)
        ]

    for j in range(chunks):
        for copy, onward in zip(own_copies(j), mate_copies(j)):
            copy.wait_recv()
            onward.start()

    eye = (
        lax.broadcasted_iota(jnp.int32, (orbitals, orbitals), 0)
        == lax.broadcasted_iota(jnp.int32, (orbitals, orbitals), 1)
    ).astype(BF16)
    my_rows = pl.ds(pl.multiple_of(q * share, share), share)

    def mix_copies(j, c):
        copies = []
        for e in range(1, wide):
            to = lax.rem(q + e, wide)
            copies.append(
                send(
                    mix.at[j, c, pl.ds(pl.multiple_of(to * share, share), share)],
                    row_mix.at[j, q, c],
                    mix_s.at[e - 1, j, c],
                    mix_r.at[e - 1, j, c],
                    s,
                    to,
                )
            )
        return copies

    def term_two(j):
        def wait_one(c, carry):
            for copy in one_copies(j, c):
                copy.wait()
            return carry

        def body(c, carry):
            right = jnp.concatenate([one_t[j][slot_ref[c, k]] for k in range(slots)], axis=0)
            term = jnp.dot(scaled[c], right, preferred_element_type=F32)
            probe = lax.dot_general(
                eye, near[j][count + c], (((1,), (1,)), ((), ())), preferred_element_type=F32
            )
            second = 2.0 * term - probe
            mix[j, c] = (
                COEFF_ZERO * probe + COEFF_ONE * first[j, c] + COEFF_TWO * second
            ).astype(BF16)
            row_mix[j, q, c] = mix[j, c, my_rows, :]
            for copy in mix_copies(j, c):
                copy.start()
            return carry

        lax.fori_loop(0, count, wait_one, 0)
        lax.fori_loop(0, count, body, 0, unroll=4)

    def overlap(j):
        def wait_mix(c, carry):
            for copy in mix_copies(j, c):
                copy.wait()
            return carry

        def body(t, carry):
            left = jnp.concatenate(
                [row_mix[j, lax.rem(q + wide - w, wide)] for w in range(wide)], axis=2
            ).reshape(count * share, wide * width)
            right = jnp.concatenate(
                [
                    jnp.concatenate([source[2 * t], source[2 * t + 1]], axis=1)
                    for source in [near[j]] + [rest[j].at[w - 1] for w in range(1, wide)]
                ],
                axis=0,
            )
            product = jnp.dot(left, right, preferred_element_type=F32)
            for h in range(2):
                value = product[:, h * orbitals : (h + 1) * orbitals].reshape(
                    count, share, orbitals
                )
                dense[2 * t + h] = value if j == 0 else dense[2 * t + h] + value
            return carry

        for copy in forward(j) + mate_copies(j):
            copy.wait_recv()
        lax.fori_loop(0, count, wait_mix, 0)
        lax.fori_loop(0, 3 * count // 2, body, 0, unroll=4)

    for j in range(chunks):
        term_two(j)
    for j in range(chunks):
        overlap(j)

    padded = col_force.shape[1]

    def forces(c, carry):
        acc = [jnp.zeros((share, orbitals), F32) for _ in range(3)]
        for k in range(slots):
            sample = dense[slot_ref[c, k], c]
            for m in range(3):
                value = sample * slope[c, k, m]
                acc[m] = acc[m] + value
                col_force[c, k, m] = jnp.sum(
                    value.reshape(share // 8, 8, orbitals), axis=0
                )
        for m in range(3):
            row_force[m, c] = jnp.sum(acc[m].reshape(turns, height, orbitals), axis=0)
        return carry

    for k in range(slots, padded):
        for c in range(count):
            for m in range(3):
                col_force[c, k, m] = jnp.zeros((8, orbitals), F32)
    lax.fori_loop(0, count, forces, 0)

    ids = lax.broadcasted_iota(jnp.int32, (3 * count, slots), 0)
    held_ids = jnp.where(
        ids < count,
        ids + down * count,
        jnp.where(ids < 2 * count, ids - count + s * count, ids - 2 * count + up * count),
    )
    blank = jnp.zeros((3 * count, padded - slots), F32)
    picked = jnp.concatenate(
        [
            part
            for c in range(count)
            for part in (
                jnp.where(wanted_ref[c : c + 1, :] == held_ids, 1.0, 0.0),
                blank,
            )
        ],
        axis=1,
    )
    for m in range(3):
        column = jnp.sum(
            col_force[:, :, m].reshape(count * padded, 8, orbitals), axis=1
        )
        moved = jnp.dot(
            picked, column, precision=lax.Precision.HIGHEST, preferred_element_type=F32
        )
        pull[m] = fold(moved)
        line = jnp.sum(row_force[m], axis=2, keepdims=True) * hit
        pull[m, own] = pull[m, own] - jnp.sum(line, axis=1)
    arrived[1, q] = pull[:, own]
    pull_out = []
    for e in range(wide):
        to = lax.rem(q + e, wide)
        moves = [(pull.at[:, after], 0, up), (pull.at[:, before], 2, down)]
        if e > 0:
            moves.append((pull.at[:, own], 1, s))
        for src, kind, to_space in moves:
            copy = send(
                src, arrived.at[kind, q], pull_s.at[kind, e], pull_r.at[kind, e], to_space, to
            )
            copy.start()
            pull_out.append(copy)

    def density(k, carry):
        for c in range(count):
            sample = dense[slot_ref[c, k], c] * (alive_ref[c, k] * scale)
            stage[pl.ds(c, share, stride=count), :] = sample
        dens_ref[:, k] = stage[...].reshape(share, count, orbitals).astype(dens_ref.dtype)
        return carry

    lax.fori_loop(0, slots, density, 0)
    for copy in pull_out:
        copy.wait()
    result = None
    for kind in range(3):
        for w in range(wide):
            part = arrived[kind, w]
            result = part if result is None else result + part
    force_ref[...] = (result * (-1.0 / total))[:, :, :atoms]

    sent = [pos_up, pos_down]
    for j in range(chunks):
        sent = sent + probe_copies(j) + own_copies(j) + forward(j) + mate_copies(j)
    for copy in sent:
        copy.wait_send()


def write_out(pieces, dens_in, force_in, dens_out, force_out, sems):
    rows = dens_in.shape[0] // pieces
    copies = [pltpu.make_async_copy(force_in, force_out, sems.at[pieces])]
    for i in range(pieces):
        part = pl.ds(i * rows, rows)
        copies.append(pltpu.make_async_copy(dens_in.at[part], dens_out.at[part], sems.at[i]))
    for copy in copies:
        copy.start()
    for copy in copies:
        copy.wait()


def per_device(positions, probes, neighbours):
    count, _, atoms = positions.shape
    slots = neighbours.shape[1]
    orbitals = 4 * atoms
    span = probes.shape[1]
    space = lax.axis_size("space")
    wide = lax.axis_size("probe")
    share = orbitals // wide
    vmem = pl.BlockSpec(memory_space=pltpu.VMEM)
    dma = pltpu.SemaphoreType.DMA
    peers = max(wide - 1, 1)
    chunks = 2 if span % (2 * LANES) == 0 else 1
    plane = 2 ** ((space.bit_length() - 1) // 2)
    pairs = plane + space // plane - 2
    width = span // chunks
    sizes = (space, wide, count, atoms, slots, span, share, chunks, plane)
    density, force = pl.pallas_call(
        functools.partial(kernel, sizes),
        name="band_forces",
        out_shape=(
            pltpu.VMEM((share, slots, count, orbitals), BF16),
            pltpu.VMEM((3, count, atoms), F32),
        ),
        in_specs=[pl.BlockSpec(memory_space=pl.ANY)] * 3,
        out_specs=(vmem, vmem),
        scratch_shapes=[
            pltpu.SMEM((count, slots), jnp.int32),
            pltpu.SMEM((count, slots), jnp.int32),
            pltpu.SMEM((count, slots), F32),
            pltpu.VMEM((count, slots), jnp.int32),
            pltpu.VMEM((3, 3, count, atoms), BF16),
            pltpu.VMEM((count, 3, atoms, orbitals), F32),
            [pltpu.VMEM((3 * count, width, orbitals), BF16)] * chunks,
            [pltpu.VMEM((peers, 3 * count, width, orbitals), BF16)] * chunks,
            pltpu.VMEM((3, 3 * count, orbitals), F32),
            pltpu.VMEM((count, orbitals, slots * orbitals), F32),
            pltpu.VMEM((count, orbitals, slots * orbitals), BF16),
            pltpu.VMEM((count, slots, 7, atoms, orbitals), F32),
            pltpu.VMEM((2, 8, LANES), F32),
            pltpu.VMEM((pairs, 8, LANES), F32),
            pltpu.VMEM((count, slots, 3, share, orbitals), F32),
            pltpu.VMEM((chunks, count, orbitals, width), F32),
            [pltpu.VMEM((3 * count, orbitals, width), BF16)] * chunks,
            pltpu.VMEM((chunks, count, orbitals, width), BF16),
            pltpu.VMEM((chunks, wide, count, share, width), BF16),
            pltpu.VMEM((3 * count, count, share, orbitals), F32),
            pltpu.VMEM((share * count, orbitals), F32),
            pltpu.VMEM((count, -(-slots // 8) * 8, 3, 8, orbitals), F32),
            pltpu.VMEM((3, count, min(atoms, share), orbitals), F32),
            pltpu.VMEM((3, 3 * count, orbitals), F32),
            pltpu.VMEM((3, wide, 3, count, orbitals), F32),
            dma((3 + chunks,)),
            dma((2,)),
            dma((2,)),
            dma((2, chunks)),
            dma((2, chunks)),
            dma((peers, chunks)),
            dma((peers, chunks)),
            dma((peers, chunks)),
            dma((peers, chunks)),
            dma((peers, chunks)),
            dma((peers, chunks)),
            dma((pairs,)),
            dma((pairs,)),
            dma((2, chunks, count)),
            dma((2, chunks, count)),
            dma((peers, chunks, count)),
            dma((peers, chunks, count)),
            dma((3, wide)),
            dma((3, wide)),
        ],
        compiler_params=pltpu.CompilerParams(
            collective_id=0, has_side_effects=True, vmem_limit_bytes=60 * 1024 * 1024
        ),
    )(neighbours, jnp.transpose(positions, (1, 0, 2)), probes)
    anywhere = pl.BlockSpec(memory_space=pl.ANY)
    density, force = pl.pallas_call(
        functools.partial(write_out, PIECES),
        name="write_out",
        out_shape=(
            jax.ShapeDtypeStruct(density.shape, BF16),
            jax.ShapeDtypeStruct(force.shape, F32),
        ),
        in_specs=[vmem, vmem],
        out_specs=(anywhere, anywhere),
        scratch_shapes=[dma((PIECES + 1,))],
        compiler_params=pltpu.CompilerParams(vmem_limit_bytes=1024 * 1024),
    )(density, force)
    return jnp.transpose(density, (0, 2, 1, 3)), jnp.transpose(force, (1, 0, 2))


def solution(mesh):
    in_specs = (P("space", None, None), P("space", "probe", None), P("space", None))
    out_specs = (P("probe", "space", None, None), P("space", None, None))
    return jax.shard_map(
        per_device, mesh=mesh, in_specs=in_specs, out_specs=out_specs, check_vma=False
    )
```

```python
import functools

import jax
import jax.numpy as jnp
from jax import lax
from jax.experimental import pallas as pl
from jax.experimental.pallas import tpu as pltpu
from jax.sharding import PartitionSpec as P

SS_SIGMA = -1.938
SP_SIGMA = 1.745
PP_SIGMA = 3.05
PP_PI = -1.075
PP_DIFF = PP_SIGMA - PP_PI
BOND_LENGTH = 2.35
SOFT_SQUARE = 0.25
CELL_EDGE = 10.86
COEFF_ZERO = 0.6
COEFF_ONE = -0.7
COEFF_TWO = 0.45
MESH = pl.DeviceIdType.MESH
LANES = 128
F32 = jnp.float32
BF16 = jnp.bfloat16


def offsets():
    half = CELL_EDGE / 2.0
    table = [(0.0, 0.0, 0.0)]
    for x in (-1.0, 1.0):
        for y in (-1.0, 1.0):
            for z in (-1.0, 1.0):
                table.append((x * half, y * half, z * half))
    for axis in range(3):
        for sign in (1.0, -1.0):
            entry = [0.0, 0.0, 0.0]
            entry[axis] = sign * CELL_EDGE
            table.append(tuple(entry))
    return table


SHIFTS = offsets()
PIECES = 8
EARLY_BUILD = 3
EARLY_SLOPES = 2


def kernel(
    sizes,
    neighbours_ref,
    positions_ref,
    probes_ref,
    dens_ref,
    force_ref,
    names_ref,
    slot_ref,
    alive_ref,
    wanted_ref,
    raw_pos,
    posc_ref,
    near,
    rest,
    near_pos,
    ham,
    scaled,
    pair,
    top_out,
    top_in,
    slope,
    first,
    one_t,
    mix,
    row_mix,
    dense,
    stage,
    col_force,
    row_force,
    pull,
    arrived,
    local_sem,
    pos_s,
    pos_r,
    probe_s,
    probe_r,
    own_s,
    own_r,
    fwd_s,
    fwd_r,
    chip_s,
    chip_r,
    yonder_s,
    yonder_r,
    max_s,
    max_r,
    one_s,
    one_r,
    mix_s,
    mix_r,
    pull_s,
    pull_r,
):
    space, wide, count, atoms, slots, span, share, chunks, plane = sizes
    width = span // chunks
    orbitals = 4 * atoms
    total = span * wide
    s = lax.axis_index("space")
    q = lax.axis_index("probe")
    up = lax.rem(s + 1, space)
    down = lax.rem(s + space - 1, space)
    before, own, after = pl.ds(0, count), pl.ds(count, count), pl.ds(2 * count, count)
    core = lax.rem(s, 2)
    mate = s + 1 - 2 * core
    far_side = pl.ds(core * (2 * count), count)

    def send(src, dst, ss, rs, to_space, to_probe):
        return pltpu.make_async_remote_copy(
            src_ref=src,
            dst_ref=dst,
            send_sem=ss,
            recv_sem=rs,
            device_id={"space": to_space, "probe": to_probe},
            device_id_type=MESH,
        )

    low, high = lax.rem(s, plane), lax.div(s, plane)
    planes = space // plane
    beside = [high * plane + lax.rem(low + d, plane) for d in range(1, plane)]
    across = [lax.rem(high + d, planes) * plane + low for d in range(1, planes)]

    barrier = pltpu.get_barrier_semaphore()

    def greet(to_space, to_probe):
        pl.semaphore_signal(
            barrier,
            inc=1,
            device_id={"space": to_space, "probe": to_probe},
            device_id_type=MESH,
        )

    for to in beside + across + [up, down]:
        greet(to, q)
    for e in range(1, wide):
        greet(s, lax.rem(q + e, wide))

    loads = [
        pltpu.make_async_copy(src, dst, local_sem.at[i])
        for i, (src, dst) in enumerate(
            [
                (positions_ref, raw_pos.at[1]),
                (neighbours_ref, names_ref),
                (neighbours_ref, wanted_ref),
            ]
            + [
                (probes_ref.at[:, pl.ds(j * width, width)], near[j].at[own])
                for j in range(chunks)
            ]
        )
    ]
    for load in loads:
        load.start()
    pl.semaphore_wait(barrier, plane + planes + wide - 1)

    pos_up = send(positions_ref, raw_pos.at[0], pos_s.at[0], pos_r.at[0], up, q)
    pos_down = send(positions_ref, raw_pos.at[2], pos_s.at[1], pos_r.at[1], down, q)
    pos_up.start()
    pos_down.start()
    half = count // 2

    def probe_copies(j, halves=(0, 1)):
        part = pl.ds(j * width, width)
        return [
            send(
                probes_ref.at[pl.ds(h * half, half), part],
                near[j].at[pl.ds(place + h * half, half)],
                probe_s.at[i, j, h],
                probe_r.at[i, j, h],
                to,
                q,
            )
            for i, (place, to) in enumerate([(0, up), (2 * count, down)])
            for h in halves
        ]

    crossing = jnp.logical_or(lax.rem(s, 4) == 0, lax.rem(s, 4) == 3)

    def start_probes(when, j, halves=(0, 1)):
        @pl.when(when)
        def _():
            for copy in probe_copies(j, halves):
                copy.start()

    start_probes(jnp.logical_not(crossing), 0, (0,))
    def own_copies(j):
        return [
            send(
                probes_ref.at[:, pl.ds(j * width, width)],
                rest[j].at[e - 1, own],
                own_s.at[e - 1, j],
                own_r.at[e - 1, j],
                s,
                lax.rem(q + e, wide),
            )
            for e in range(1, wide)
        ]

    for j in range(chunks):
        for copy in own_copies(j):
            copy.start()

    def fold(x):
        return (
            x
            + pltpu.roll(x, atoms, 1)
            + pltpu.roll(x, 2 * atoms, 1)
            + pltpu.roll(x, 3 * atoms, 1)
        )

    def spread(part):
        rows = pl.ds(part * count, count)
        for m in range(3):
            near_pos[m, rows, :atoms] = raw_pos[part, m].astype(F32)
            near_pos[m, rows] = fold(jnp.where(narrow, near_pos[m, rows], 0.0))

    for load in loads[:3]:
        load.wait()
    narrow = lax.broadcasted_iota(jnp.int32, (count, orbitals), 1) < atoms
    spread(1)
    for m in range(3):
        tall = jnp.transpose(near_pos[m, own])
        for c in range(count):
            posc_ref[c, m] = jnp.broadcast_to(tall[:atoms, c : c + 1], (atoms, orbitals))

    def find_slots(c, carry):
        for k in range(slots):
            name = names_ref[c, k]
            held = jnp.maximum(name, 0)
            place = lax.rem(lax.div(held, count) - s + 1 + space, space) * count
            place = place + lax.rem(held, count)
            slot_ref[c, k] = jnp.where(name >= 0, jnp.minimum(place, 3 * count - 1), count)
            alive_ref[c, k] = jnp.where(name >= 0, 1.0, 0.0)
        return carry

    lax.fori_loop(0, count, find_slots, 0)
    start_probes(crossing, 0)
    pos_up.wait_recv()
    spread(0)
    pos_down.wait_recv()
    spread(2)

    lane = lax.broadcasted_iota(jnp.int32, (atoms, orbitals), 1)
    group = lane // atoms
    is_s = group == 0
    is_p = [group == 1, group == 2, group == 3]
    pp = [jnp.where(m, PP_PI, 0.0).astype(F32) for m in is_p]

    def peak_of(c, peak):
        rows = [posc_ref[c, m] for m in range(3)]
        sums = [jnp.zeros((atoms, orbitals), F32) for _ in range(4)]
        for k in range(0, slots, 4):
            picked = range(k, min(k + 4, slots))
            alive = jnp.zeros((1, orbitals), F32)
            column = [jnp.zeros((1, orbitals), F32) for _ in range(3)]
            for i, t in enumerate(picked):
                here = group[:1] == i
                alive = jnp.where(here, alive_ref[c, t], alive)
                place = slot_ref[c, t]
                for m in range(3):
                    column[m] = jnp.where(
                        here, near_pos[m, pl.ds(place, 1), :] + SHIFTS[t][m], column[m]
                    )
            d = [column[m] - rows[m] for m in range(3)]
            square = d[0] * d[0] + d[1] * d[1] + d[2] * d[2] + SOFT_SQUARE
            inv = lax.rsqrt(square)
            u = [jnp.abs(x) * inv for x in d]
            g = jnp.exp(1.0 - square * (1.0 / (BOND_LENGTH * BOND_LENGTH))) * alive
            sums[0] = sums[0] + g * ((u[0] + u[1] + u[2]) * SP_SIGMA - SS_SIGMA)
            for a in range(3):
                others = u[(a + 1) % 3] + u[(a + 2) % 3]
                value = u[a] * (others * PP_DIFF + SP_SIGMA)
                value = value + jnp.abs(u[a] * u[a] * PP_DIFF + PP_PI)
                sums[1 + a] = sums[1 + a] + g * value
        for a in range(4):
            peak = jnp.maximum(peak, jnp.sum(sums[a], axis=1, keepdims=True))
        return peak

    def build(c, carry):
        rows = [posc_ref[c, m] for m in range(3)]
        for k in range(slots):
            place = slot_ref[c, k]
            alive = alive_ref[c, k]
            d = [
                (near_pos[m, pl.ds(place, 1), :] + SHIFTS[k][m]) - rows[m] for m in range(3)
            ]
            square = d[0] * d[0] + d[1] * d[1] + d[2] * d[2] + SOFT_SQUARE
            inv = lax.rsqrt(square)
            l = [x * inv for x in d]
            g = jnp.exp(1.0 - square * (1.0 / (BOND_LENGTH * BOND_LENGTH))) * alive
            beta = jnp.where(
                is_s, 0.0, jnp.where(is_p[0], l[0], jnp.where(is_p[1], l[1], l[2]))
            )
            coef_s = jnp.where(is_s, SS_SIGMA, SP_SIGMA * beta)
            coef_p = jnp.where(is_s, -SP_SIGMA, PP_DIFF * beta)
            parts = [coef_s * g] + [(l[m] * coef_p + pp[m]) * g for m in range(3)]
            for a in range(4):
                ham[c, a * atoms : (a + 1) * atoms, k * orbitals : (k + 1) * orbitals] = parts[a]
            pair[c, k, 0] = jnp.zeros_like(g)
            for m in range(3):
                pair[c, k, 1 + m] = l[m]
            pair[c, k, 4] = beta
            pair[c, k, 5] = g * inv
            pair[c, k, 6] = g * (square * inv) * (2.0 / (BOND_LENGTH * BOND_LENGTH))
        return carry

    height = min(atoms, share)
    turns = share // height
    start_atom = lax.rem(q * share, atoms)
    rows = pl.ds(pl.multiple_of(start_atom, height), height)
    s_mask = jnp.where(is_s[:height], 1.0, 0.0).astype(F32)
    p_mask = [jnp.where(m[:height], 1.0, 0.0).astype(F32) for m in is_p]
    row_iota = lax.broadcasted_iota(jnp.int32, (height, orbitals), 0) + start_atom
    hit = jnp.where(row_iota == lax.rem(lane[:height], atoms), 1.0, 0.0).astype(F32)
    scale = 1.0 / float(total) ** 0.5

    def slopes(c, carry):
        for t in range(turns):
            kind = (q * share) // atoms + t
            ws = jnp.where(kind == 0, 1.0, 0.0).astype(F32)
            wr = [jnp.where(kind == m + 1, 1.0, 0.0).astype(F32) for m in range(3)]
            wv = PP_PI * (wr[0] * p_mask[0] + wr[1] * p_mask[1] + wr[2] * p_mask[2])
            wv = wv + (ws * SS_SIGMA) * s_mask
            for k in range(slots):
                alpha = pair[c, k, kind, rows, :]
                beta = pair[c, k, 4, rows, :]
                lean = pair[c, k, 5, rows, :]
                c_one = PP_DIFF * alpha + ws * SP_SIGMA
                c_two = PP_DIFF * beta - SP_SIGMA * s_mask
                cross = alpha * c_two
                bracket = (ws * SP_SIGMA) * beta + cross + wv
                x = lean * c_one
                y = lean * c_two
                drag = lean * (c_one * beta + cross) + pair[c, k, 6, rows, :] * bracket
                for m in range(3):
                    slope[c, k, m, t * height : (t + 1) * height] = (
                        x * p_mask[m] + y * wr[m] - drag * pair[c, k, 1 + m, rows, :]
                    )
        return carry

    peak = lax.fori_loop(0, count, peak_of, jnp.zeros((atoms, 1), F32), unroll=2)
    top = jnp.broadcast_to(jnp.max(peak, axis=0, keepdims=True), (8, LANES))

    def top_copies(stage, devices):
        base = 0 if stage == 0 else plane - 1
        return [
            send(
                top_out.at[stage],
                top_in.at[base + i],
                max_s.at[base + i],
                max_r.at[base + i],
                to,
                q,
            )
            for i, to in enumerate(devices)
        ]

    def raise_top(top, stage, devices):
        base = 0 if stage == 0 else plane - 1
        for i, copy in enumerate(top_copies(stage, devices)):
            copy.wait()
            top = jnp.maximum(top, top_in[base + i])
        return top

    last = chunks - 1

    def forward(j):
        copies = []
        far_part = pl.ds(core * (2 * count), half if j == last else count)
        for e in range(1, wide):
            copies.append(
                send(
                    near[j].at[far_part],
                    rest[j].at[e - 1, far_part],
                    fwd_s.at[e - 1, j],
                    fwd_r.at[e - 1, j],
                    s,
                    lax.rem(q + e, wide),
                )
            )
        return copies

    top_out[0] = top
    for copy in top_copies(0, beside):
        copy.start()
    start_probes(jnp.logical_not(crossing), 0, (1,))
    for j in range(1, chunks):
        start_probes(jnp.logical_not(crossing), j)
    lax.fori_loop(0, EARLY_BUILD, build, 0)
    top = raise_top(top, 0, beside)
    top_out[1] = top
    for copy in top_copies(1, across):
        copy.start()
    for j in range(1, chunks):
        start_probes(crossing, j)
    lax.fori_loop(EARLY_BUILD, count, build, 0)
    lax.fori_loop(0, EARLY_SLOPES, slopes, 0)
    for load in loads[3:]:
        load.wait()
    for copy in probe_copies(0):
        copy.wait_recv()
    for copy in forward(0):
        copy.start()
    top = raise_top(top, 1, across)
    shrink = 1.0 / top[0:1]

    def one_copies(j, c):
        return [
            send(
                one_t[j].at[count + c],
                one_t[j].at[place + c],
                one_s.at[i, j, c],
                one_r.at[i, j, c],
                to,
                q,
            )
            for i, (place, to) in enumerate([(0, up), (2 * count, down)])
        ]

    def term_one(j):
        def body(c, carry):
            if j == 0:
                for k in range(slots):
                    here = pl.ds(k * orbitals, orbitals)
                    scaled[c, :, here] = (ham[c, :, here] * shrink).astype(BF16)
            right = jnp.concatenate([near[j][slot_ref[c, k]] for k in range(slots)], axis=1)
            term = lax.dot_general(
                scaled[c], right, (((1,), (1,)), ((), ())), preferred_element_type=F32
            )
            first[j, c] = term
            one_t[j][count + c] = term.astype(BF16)
            for copy in one_copies(j, c):
                copy.start()
            return carry

        lax.fori_loop(0, count, body, 0)

    term_one(0)
    def later_slopes(when):
        @pl.when(when)
        def _():
            lax.fori_loop(EARLY_SLOPES, count, slopes, 0)

    for j in range(1, chunks):
        for copy in probe_copies(j):
            copy.wait_recv()
        for copy in forward(j):
            copy.start()
    later_slopes(crossing)
    for j in range(1, chunks):
        term_one(j)
    later_slopes(jnp.logical_not(crossing))

    def mate_copies(j):
        return [
            send(
                rest[j].at[e - 1, own],
                rest[j].at[e - 1, far_side],
                chip_s.at[e - 1, j],
                chip_r.at[e - 1, j],
                mate,
                q,
            )
            for e in range(1, wide)
        ]

    far_to = core * up + (1 - core) * down
    yonder = [
        send(
            rest[last].at[e - 1, pl.ds(count + half, half)],
            rest[last].at[e - 1, pl.ds((1 - core) * (2 * count) + half, half)],
            yonder_s.at[e - 1],
            yonder_r.at[e - 1],
            far_to,
            q,
        )
        for e in range(1, wide)
    ]

    for j in range(chunks):
        for copy, onward in zip(own_copies(j), mate_copies(j)):
            copy.wait_recv()
            onward.start()

    eye = (
        lax.broadcasted_iota(jnp.int32, (orbitals, orbitals), 0)
        == lax.broadcasted_iota(jnp.int32, (orbitals, orbitals), 1)
    ).astype(BF16)
    my_rows = pl.ds(pl.multiple_of(q * share, share), share)

    def mix_copies(j, c):
        copies = []
        for e in range(1, wide):
            to = lax.rem(q + e, wide)
            copies.append(
                send(
                    mix.at[j, c, pl.ds(pl.multiple_of(to * share, share), share)],
                    row_mix.at[j, q, c],
                    mix_s.at[e - 1, j, c],
                    mix_r.at[e - 1, j, c],
                    s,
                    to,
                )
            )
        return copies

    def term_two(j):
        def wait_one(c, carry):
            for copy in one_copies(j, c):
                copy.wait()
            return carry

        def body(c, carry):
            right = jnp.concatenate([one_t[j][slot_ref[c, k]] for k in range(slots)], axis=0)
            term = jnp.dot(scaled[c], right, preferred_element_type=F32)
            probe = lax.dot_general(
                eye, near[j][count + c], (((1,), (1,)), ((), ())), preferred_element_type=F32
            )
            second = 2.0 * term - probe
            mix[j, c] = (
                COEFF_ZERO * probe + COEFF_ONE * first[j, c] + COEFF_TWO * second
            ).astype(BF16)
            row_mix[j, q, c] = mix[j, c, my_rows, :]
            for copy in mix_copies(j, c):
                copy.start()
            return carry

        lax.fori_loop(0, count, wait_one, 0)
        if j == last:
            for copy in yonder:
                copy.start()
        lax.fori_loop(0, count, body, 0, unroll=4)

    def overlap(j):
        def wait_mix(c, carry):
            for copy in mix_copies(j, c):
                copy.wait()
            return carry

        def body(t, carry):
            left = jnp.concatenate(
                [row_mix[j, lax.rem(q + wide - w, wide)] for w in range(wide)], axis=2
            ).reshape(count * share, wide * width)
            right = jnp.concatenate(
                [
                    jnp.concatenate([source[2 * t], source[2 * t + 1]], axis=1)
                    for source in [near[j]] + [rest[j].at[w - 1] for w in range(1, wide)]
                ],
                axis=0,
            )
            product = jnp.dot(left, right, preferred_element_type=F32)
            for h in range(2):
                value = product[:, h * orbitals : (h + 1) * orbitals].reshape(
                    count, share, orbitals
                )
                dense[2 * t + h] = value if j == 0 else dense[2 * t + h] + value
            return carry

        for copy in forward(j) + mate_copies(j) + (yonder if j == last else []):
            copy.wait_recv()
        lax.fori_loop(0, count, wait_mix, 0)
        lax.fori_loop(0, 3 * count // 2, body, 0, unroll=4)

    for j in range(chunks):
        term_two(j)
    for j in range(chunks):
        overlap(j)

    padded = col_force.shape[1]

    def forces(c, carry):
        acc = [jnp.zeros((share, orbitals), F32) for _ in range(3)]
        for k in range(slots):
            sample = dense[slot_ref[c, k], c]
            for m in range(3):
                value = sample * slope[c, k, m]
                acc[m] = acc[m] + value
                col_force[c, k, m] = jnp.sum(
                    value.reshape(share // 8, 8, orbitals), axis=0
                )
        for m in range(3):
            row_force[m, c] = jnp.sum(acc[m].reshape(turns, height, orbitals), axis=0)
        return carry

    for k in range(slots, padded):
        for c in range(count):
            for m in range(3):
                col_force[c, k, m] = jnp.zeros((8, orbitals), F32)
    lax.fori_loop(0, count, forces, 0)

    ids = lax.broadcasted_iota(jnp.int32, (3 * count, slots), 0)
    held_ids = jnp.where(
        ids < count,
        ids + down * count,
        jnp.where(ids < 2 * count, ids - count + s * count, ids - 2 * count + up * count),
    )
    blank = jnp.zeros((3 * count, padded - slots), F32)
    picked = jnp.concatenate(
        [
            part
            for c in range(count)
            for part in (
                jnp.where(wanted_ref[c : c + 1, :] == held_ids, 1.0, 0.0),
                blank,
            )
        ],
        axis=1,
    )
    for m in range(3):
        column = jnp.sum(
            col_force[:, :, m].reshape(count * padded, 8, orbitals), axis=1
        )
        moved = jnp.dot(
            picked, column, precision=lax.Precision.HIGHEST, preferred_element_type=F32
        )
        pull[m] = fold(moved)
        line = jnp.sum(row_force[m], axis=2, keepdims=True) * hit
        pull[m, own] = pull[m, own] - jnp.sum(line, axis=1)
    arrived[1, q] = pull[:, own]
    pull_out = []
    for e in range(wide):
        to = lax.rem(q + e, wide)
        moves = [(pull.at[:, after], 0, up), (pull.at[:, before], 2, down)]
        if e > 0:
            moves.append((pull.at[:, own], 1, s))
        for src, kind, to_space in moves:
            copy = send(
                src, arrived.at[kind, q], pull_s.at[kind, e], pull_r.at[kind, e], to_space, to
            )
            copy.start()
            pull_out.append(copy)

    def density(k, carry):
        for c in range(count):
            sample = dense[slot_ref[c, k], c] * (alive_ref[c, k] * scale)
            stage[pl.ds(c, share, stride=count), :] = sample
        dens_ref[:, k] = stage[...].reshape(share, count, orbitals).astype(dens_ref.dtype)
        return carry

    lax.fori_loop(0, slots, density, 0)
    for copy in pull_out:
        copy.wait()
    result = None
    for kind in range(3):
        for w in range(wide):
            part = arrived[kind, w]
            result = part if result is None else result + part
    force_ref[...] = (result * (-1.0 / total))[:, :, :atoms]

    sent = [pos_up, pos_down] + yonder
    for j in range(chunks):
        sent = sent + probe_copies(j) + own_copies(j) + forward(j) + mate_copies(j)
    for copy in sent:
        copy.wait_send()


def write_out(pieces, dens_in, force_in, dens_out, force_out, sems):
    rows = dens_in.shape[0] // pieces
    copies = [pltpu.make_async_copy(force_in, force_out, sems.at[pieces])]
    for i in range(pieces):
        part = pl.ds(i * rows, rows)
        copies.append(pltpu.make_async_copy(dens_in.at[part], dens_out.at[part], sems.at[i]))
    for copy in copies:
        copy.start()
    for copy in copies:
        copy.wait()


def per_device(positions, probes, neighbours):
    count, _, atoms = positions.shape
    slots = neighbours.shape[1]
    orbitals = 4 * atoms
    span = probes.shape[1]
    space = lax.axis_size("space")
    wide = lax.axis_size("probe")
    share = orbitals // wide
    vmem = pl.BlockSpec(memory_space=pltpu.VMEM)
    dma = pltpu.SemaphoreType.DMA
    peers = max(wide - 1, 1)
    chunks = 2 if span % (2 * LANES) == 0 else 1
    plane = 2 ** ((space.bit_length() - 1) // 2)
    pairs = plane + space // plane - 2
    width = span // chunks
    sizes = (space, wide, count, atoms, slots, span, share, chunks, plane)
    density, force = pl.pallas_call(
        functools.partial(kernel, sizes),
        name="band_forces",
        out_shape=(
            pltpu.VMEM((share, slots, count, orbitals), BF16),
            pltpu.VMEM((3, count, atoms), F32),
        ),
        in_specs=[pl.BlockSpec(memory_space=pl.ANY)] * 3,
        out_specs=(vmem, vmem),
        scratch_shapes=[
            pltpu.SMEM((count, slots), jnp.int32),
            pltpu.SMEM((count, slots), jnp.int32),
            pltpu.SMEM((count, slots), F32),
            pltpu.VMEM((count, slots), jnp.int32),
            pltpu.VMEM((3, 3, count, atoms), BF16),
            pltpu.VMEM((count, 3, atoms, orbitals), F32),
            [pltpu.VMEM((3 * count, width, orbitals), BF16)] * chunks,
            [pltpu.VMEM((peers, 3 * count, width, orbitals), BF16)] * chunks,
            pltpu.VMEM((3, 3 * count, orbitals), F32),
            pltpu.VMEM((count, orbitals, slots * orbitals), F32),
            pltpu.VMEM((count, orbitals, slots * orbitals), BF16),
            pltpu.VMEM((count, slots, 7, atoms, orbitals), F32),
            pltpu.VMEM((2, 8, LANES), F32),
            pltpu.VMEM((pairs, 8, LANES), F32),
            pltpu.VMEM((count, slots, 3, share, orbitals), F32),
            pltpu.VMEM((chunks, count, orbitals, width), F32),
            [pltpu.VMEM((3 * count, orbitals, width), BF16)] * chunks,
            pltpu.VMEM((chunks, count, orbitals, width), BF16),
            pltpu.VMEM((chunks, wide, count, share, width), BF16),
            pltpu.VMEM((3 * count, count, share, orbitals), F32),
            pltpu.VMEM((share * count, orbitals), F32),
            pltpu.VMEM((count, -(-slots // 8) * 8, 3, 8, orbitals), F32),
            pltpu.VMEM((3, count, min(atoms, share), orbitals), F32),
            pltpu.VMEM((3, 3 * count, orbitals), F32),
            pltpu.VMEM((3, wide, 3, count, orbitals), F32),
            dma((3 + chunks,)),
            dma((2,)),
            dma((2,)),
            dma((2, chunks, 2)),
            dma((2, chunks, 2)),
            dma((peers, chunks)),
            dma((peers, chunks)),
            dma((peers, chunks)),
            dma((peers, chunks)),
            dma((peers, chunks)),
            dma((peers, chunks)),
            dma((peers,)),
            dma((peers,)),
            dma((pairs,)),
            dma((pairs,)),
            dma((2, chunks, count)),
            dma((2, chunks, count)),
            dma((peers, chunks, count)),
            dma((peers, chunks, count)),
            dma((3, wide)),
            dma((3, wide)),
        ],
        compiler_params=pltpu.CompilerParams(
            collective_id=0, has_side_effects=True, vmem_limit_bytes=60 * 1024 * 1024
        ),
    )(neighbours, jnp.transpose(positions, (1, 0, 2)), probes)
    anywhere = pl.BlockSpec(memory_space=pl.ANY)
    density, force = pl.pallas_call(
        functools.partial(write_out, PIECES),
        name="write_out",
        out_shape=(
            jax.ShapeDtypeStruct(density.shape, BF16),
            jax.ShapeDtypeStruct(force.shape, F32),
        ),
        in_specs=[vmem, vmem],
        out_specs=(anywhere, anywhere),
        scratch_shapes=[dma((PIECES + 1,))],
        compiler_params=pltpu.CompilerParams(vmem_limit_bytes=1024 * 1024),
    )(density, force)
    return jnp.transpose(density, (0, 2, 1, 3)), jnp.transpose(force, (1, 0, 2))


def solution(mesh):
    in_specs = (P("space", None, None), P("space", "probe", None), P("space", None))
    out_specs = (P("probe", "space", None, None), P("space", None, None))
    return jax.shard_map(
        per_device, mesh=mesh, in_specs=in_specs, out_specs=out_specs, check_vma=False
    )
```

```python
import functools

import jax
import jax.numpy as jnp
from jax import lax
from jax.experimental import pallas as pl
from jax.experimental.pallas import tpu as pltpu
from jax.sharding import PartitionSpec as P

SS_SIGMA = -1.938
SP_SIGMA = 1.745
PP_SIGMA = 3.05
PP_PI = -1.075
PP_DIFF = PP_SIGMA - PP_PI
BOND_LENGTH = 2.35
SOFT_SQUARE = 0.25
CELL_EDGE = 10.86
COEFF_ZERO = 0.6
COEFF_ONE = -0.7
COEFF_TWO = 0.45
MESH = pl.DeviceIdType.MESH
LANES = 128
F32 = jnp.float32
BF16 = jnp.bfloat16


def offsets():
    half = CELL_EDGE / 2.0
    table = [(0.0, 0.0, 0.0)]
    for x in (-1.0, 1.0):
        for y in (-1.0, 1.0):
            for z in (-1.0, 1.0):
                table.append((x * half, y * half, z * half))
    for axis in range(3):
        for sign in (1.0, -1.0):
            entry = [0.0, 0.0, 0.0]
            entry[axis] = sign * CELL_EDGE
            table.append(tuple(entry))
    return table


SHIFTS = offsets()
PIECES = 8
EARLY_BUILD = 3
EARLY_SLOPES = 0


def kernel(
    sizes,
    neighbours_ref,
    positions_ref,
    probes_ref,
    dens_ref,
    force_ref,
    names_ref,
    slot_ref,
    alive_ref,
    wanted_ref,
    raw_pos,
    posc_ref,
    near,
    rest,
    near_pos,
    ham,
    scaled,
    pair,
    top_out,
    top_in,
    slope,
    first,
    one_t,
    mix,
    row_mix,
    dense,
    stage,
    col_force,
    row_force,
    pull,
    arrived,
    local_sem,
    pos_s,
    pos_r,
    probe_s,
    probe_r,
    own_s,
    own_r,
    fwd_s,
    fwd_r,
    chip_s,
    chip_r,
    yonder_s,
    yonder_r,
    max_s,
    max_r,
    one_s,
    one_r,
    mix_s,
    mix_r,
    pull_s,
    pull_r,
):
    space, wide, count, atoms, slots, span, share, chunks, plane = sizes
    width = span // chunks
    orbitals = 4 * atoms
    total = span * wide
    s = lax.axis_index("space")
    q = lax.axis_index("probe")
    up = lax.rem(s + 1, space)
    down = lax.rem(s + space - 1, space)
    before, own, after = pl.ds(0, count), pl.ds(count, count), pl.ds(2 * count, count)
    core = lax.rem(s, 2)
    mate = s + 1 - 2 * core
    far_side = pl.ds(core * (2 * count), count)

    def send(src, dst, ss, rs, to_space, to_probe):
        return pltpu.make_async_remote_copy(
            src_ref=src,
            dst_ref=dst,
            send_sem=ss,
            recv_sem=rs,
            device_id={"space": to_space, "probe": to_probe},
            device_id_type=MESH,
        )

    low, high = lax.rem(s, plane), lax.div(s, plane)
    planes = space // plane
    beside = [high * plane + lax.rem(low + d, plane) for d in range(1, plane)]
    across = [lax.rem(high + d, planes) * plane + low for d in range(1, planes)]

    barrier = pltpu.get_barrier_semaphore()

    def greet(to_space, to_probe):
        pl.semaphore_signal(
            barrier,
            inc=1,
            device_id={"space": to_space, "probe": to_probe},
            device_id_type=MESH,
        )

    for to in beside + across + [up, down]:
        greet(to, q)
    for e in range(1, wide):
        greet(s, lax.rem(q + e, wide))

    loads = [
        pltpu.make_async_copy(src, dst, local_sem.at[i])
        for i, (src, dst) in enumerate(
            [
                (positions_ref, raw_pos.at[1]),
                (neighbours_ref, names_ref),
                (neighbours_ref, wanted_ref),
            ]
            + [
                (probes_ref.at[:, pl.ds(j * width, width)], near[j].at[own])
                for j in range(chunks)
            ]
        )
    ]
    for load in loads:
        load.start()
    pl.semaphore_wait(barrier, plane + planes + wide - 1)

    pos_up = send(positions_ref, raw_pos.at[0], pos_s.at[0], pos_r.at[0], up, q)
    pos_down = send(positions_ref, raw_pos.at[2], pos_s.at[1], pos_r.at[1], down, q)
    pos_up.start()
    pos_down.start()
    half = count // 2

    def probe_copies(j, halves=(0, 1)):
        part = pl.ds(j * width, width)
        return [
            send(
                probes_ref.at[pl.ds(h * half, half), part],
                near[j].at[pl.ds(place + h * half, half)],
                probe_s.at[i, j, h],
                probe_r.at[i, j, h],
                to,
                q,
            )
            for i, (place, to) in enumerate([(0, up), (2 * count, down)])
            for h in halves
        ]

    crossing = jnp.logical_or(lax.rem(s, 4) == 0, lax.rem(s, 4) == 3)

    def start_probes(when, j, halves=(0, 1)):
        @pl.when(when)
        def _():
            for copy in probe_copies(j, halves):
                copy.start()

    start_probes(jnp.logical_not(crossing), 0, (0,))
    def own_copies(j):
        return [
            send(
                probes_ref.at[:, pl.ds(j * width, width)],
                rest[j].at[e - 1, own],
                own_s.at[e - 1, j],
                own_r.at[e - 1, j],
                s,
                lax.rem(q + e, wide),
            )
            for e in range(1, wide)
        ]

    for copy in own_copies(0):
        copy.start()

    def fold(x):
        return (
            x
            + pltpu.roll(x, atoms, 1)
            + pltpu.roll(x, 2 * atoms, 1)
            + pltpu.roll(x, 3 * atoms, 1)
        )

    def spread(part):
        rows = pl.ds(part * count, count)
        for m in range(3):
            near_pos[m, rows, :atoms] = raw_pos[part, m].astype(F32)
            near_pos[m, rows] = fold(jnp.where(narrow, near_pos[m, rows], 0.0))

    for load in loads[:3]:
        load.wait()
    narrow = lax.broadcasted_iota(jnp.int32, (count, orbitals), 1) < atoms
    spread(1)
    for m in range(3):
        tall = jnp.transpose(near_pos[m, own])
        for c in range(count):
            posc_ref[c, m] = jnp.broadcast_to(tall[:atoms, c : c + 1], (atoms, orbitals))

    def find_slots(c, carry):
        for k in range(slots):
            name = names_ref[c, k]
            held = jnp.maximum(name, 0)
            place = lax.rem(lax.div(held, count) - s + 1 + space, space) * count
            place = place + lax.rem(held, count)
            slot_ref[c, k] = jnp.where(name >= 0, jnp.minimum(place, 3 * count - 1), count)
            alive_ref[c, k] = jnp.where(name >= 0, 1.0, 0.0)
        return carry

    lax.fori_loop(0, count, find_slots, 0)
    start_probes(crossing, 0)
    pos_up.wait_recv()
    spread(0)
    pos_down.wait_recv()
    spread(2)

    lane = lax.broadcasted_iota(jnp.int32, (atoms, orbitals), 1)
    group = lane // atoms
    is_s = group == 0
    is_p = [group == 1, group == 2, group == 3]
    pp = [jnp.where(m, PP_PI, 0.0).astype(F32) for m in is_p]

    def peak_of(c, peak):
        rows = [posc_ref[c, m] for m in range(3)]
        sums = [jnp.zeros((atoms, orbitals), F32) for _ in range(4)]
        for k in range(0, slots, 4):
            picked = range(k, min(k + 4, slots))
            alive = jnp.zeros((1, orbitals), F32)
            column = [jnp.zeros((1, orbitals), F32) for _ in range(3)]
            for i, t in enumerate(picked):
                here = group[:1] == i
                alive = jnp.where(here, alive_ref[c, t], alive)
                place = slot_ref[c, t]
                for m in range(3):
                    column[m] = jnp.where(
                        here, near_pos[m, pl.ds(place, 1), :] + SHIFTS[t][m], column[m]
                    )
            d = [column[m] - rows[m] for m in range(3)]
            square = d[0] * d[0] + d[1] * d[1] + d[2] * d[2] + SOFT_SQUARE
            inv = lax.rsqrt(square)
            u = [jnp.abs(x) * inv for x in d]
            g = jnp.exp(1.0 - square * (1.0 / (BOND_LENGTH * BOND_LENGTH))) * alive
            sums[0] = sums[0] + g * ((u[0] + u[1] + u[2]) * SP_SIGMA - SS_SIGMA)
            for a in range(3):
                others = u[(a + 1) % 3] + u[(a + 2) % 3]
                value = u[a] * (others * PP_DIFF + SP_SIGMA)
                value = value + jnp.abs(u[a] * u[a] * PP_DIFF + PP_PI)
                sums[1 + a] = sums[1 + a] + g * value
        for a in range(4):
            peak = jnp.maximum(peak, jnp.sum(sums[a], axis=1, keepdims=True))
        return peak

    def build(c, carry):
        rows = [posc_ref[c, m] for m in range(3)]
        for k in range(slots):
            place = slot_ref[c, k]
            alive = alive_ref[c, k]
            d = [
                (near_pos[m, pl.ds(place, 1), :] + SHIFTS[k][m]) - rows[m] for m in range(3)
            ]
            square = d[0] * d[0] + d[1] * d[1] + d[2] * d[2] + SOFT_SQUARE
            inv = lax.rsqrt(square)
            l = [x * inv for x in d]
            g = jnp.exp(1.0 - square * (1.0 / (BOND_LENGTH * BOND_LENGTH))) * alive
            beta = jnp.where(
                is_s, 0.0, jnp.where(is_p[0], l[0], jnp.where(is_p[1], l[1], l[2]))
            )
            coef_s = jnp.where(is_s, SS_SIGMA, SP_SIGMA * beta)
            coef_p = jnp.where(is_s, -SP_SIGMA, PP_DIFF * beta)
            parts = [coef_s * g] + [(l[m] * coef_p + pp[m]) * g for m in range(3)]
            for a in range(4):
                ham[c, a * atoms : (a + 1) * atoms, k * orbitals : (k + 1) * orbitals] = parts[a]
            pair[c, k, 0] = jnp.full_like(g, SP_SIGMA / PP_DIFF)
            for m in range(3):
                pair[c, k, 1 + m] = l[m]
            pair[c, k, 4] = coef_p
            pair[c, k, 5] = g * inv
            pair[c, k, 6] = square * inv * (2.0 / (BOND_LENGTH * BOND_LENGTH))
        return carry

    height = min(atoms, share)
    turns = share // height
    start_atom = lax.rem(q * share, atoms)
    rows = pl.ds(pl.multiple_of(start_atom, height), height)
    s_mask = jnp.where(is_s[:height], 1.0, 0.0).astype(F32)
    p_mask = [jnp.where(m[:height], 1.0, 0.0).astype(F32) for m in is_p]
    row_iota = lax.broadcasted_iota(jnp.int32, (height, orbitals), 0) + start_atom
    hit = jnp.where(row_iota == lax.rem(lane[:height], atoms), 1.0, 0.0).astype(F32)
    scale = 1.0 / float(total) ** 0.5

    def slopes(c, carry):
        for t in range(turns):
            kind = (q * share) // atoms + t
            is_row_p = jnp.where(kind > 0, 1.0, 0.0).astype(F32)
            plane_of = jnp.maximum(kind - 1, 0)
            twice = (1.0 + is_row_p) * (1.0 / PP_DIFF)
            lift = (SP_SIGMA / PP_DIFF) * s_mask
            own_rows = pl.ds(pl.multiple_of(q * share + t * height, height), height)
            part = slice(t * height, (t + 1) * height)
            for k in range(slots):
                c_two = pair[c, k, 4, rows, :]
                lean = pair[c, k, 5, rows, :]
                x = lean * (PP_DIFF * pair[c, k, kind, rows, :])
                y = lean * c_two
                block = ham[c, own_rows, k * orbitals : (k + 1) * orbitals]
                drag = x * (c_two * twice + lift) + block * pair[c, k, 6, rows, :]
                for m in range(3):
                    slope[c, k, m, part] = x * p_mask[m] - drag * pair[c, k, 1 + m, rows, :]
                slope[c, k, plane_of, part] = slope[c, k, plane_of, part] + y * is_row_p
        return carry

    peak = lax.fori_loop(0, count, peak_of, jnp.zeros((atoms, 1), F32), unroll=2)
    top = jnp.broadcast_to(jnp.max(peak, axis=0, keepdims=True), (8, LANES))

    def top_copies(stage, devices):
        base = 0 if stage == 0 else plane - 1
        return [
            send(
                top_out.at[stage],
                top_in.at[base + i],
                max_s.at[base + i],
                max_r.at[base + i],
                to,
                q,
            )
            for i, to in enumerate(devices)
        ]

    def raise_top(top, stage, devices):
        base = 0 if stage == 0 else plane - 1
        for i, copy in enumerate(top_copies(stage, devices)):
            copy.wait()
            top = jnp.maximum(top, top_in[base + i])
        return top

    last = chunks - 1

    def forward(j):
        copies = []
        far_part = pl.ds(core * (2 * count), half if j == last else count)
        for e in range(1, wide):
            copies.append(
                send(
                    near[j].at[far_part],
                    rest[j].at[e - 1, far_part],
                    fwd_s.at[e - 1, j],
                    fwd_r.at[e - 1, j],
                    s,
                    lax.rem(q + e, wide),
                )
            )
        return copies

    top_out[0] = top
    for copy in top_copies(0, beside):
        copy.start()
    start_probes(jnp.logical_not(crossing), 0, (1,))
    for j in range(1, chunks):
        start_probes(jnp.logical_not(crossing), j)
    for j in range(1, chunks):
        for copy in own_copies(j):
            copy.start()
    lax.fori_loop(0, EARLY_BUILD, build, 0)
    top = raise_top(top, 0, beside)
    top_out[1] = top
    for copy in top_copies(1, across):
        copy.start()
    for j in range(1, chunks):
        start_probes(crossing, j)
    lax.fori_loop(EARLY_BUILD, count, build, 0)
    lax.fori_loop(0, EARLY_SLOPES, slopes, 0)
    for load in loads[3:]:
        load.wait()
    for copy in probe_copies(0):
        copy.wait_recv()
    for copy in forward(0):
        copy.start()
    top = raise_top(top, 1, across)
    shrink = 1.0 / top[0:1]

    def one_copies(j, c):
        return [
            send(
                one_t[j].at[count + c],
                one_t[j].at[place + c],
                one_s.at[i, j, c],
                one_r.at[i, j, c],
                to,
                q,
            )
            for i, (place, to) in enumerate([(0, up), (2 * count, down)])
        ]

    def term_one(j):
        def body(c, carry):
            if j == 0:
                for k in range(slots):
                    here = pl.ds(k * orbitals, orbitals)
                    scaled[c, :, here] = (ham[c, :, here] * shrink).astype(BF16)
            right = jnp.concatenate([near[j][slot_ref[c, k]] for k in range(slots)], axis=1)
            term = lax.dot_general(
                scaled[c], right, (((1,), (1,)), ((), ())), preferred_element_type=F32
            )
            first[j, c] = term
            one_t[j][count + c] = term.astype(BF16)
            for copy in one_copies(j, c):
                copy.start()
            return carry

        lax.fori_loop(0, count, body, 0)

    term_one(0)
    def later_slopes(when):
        @pl.when(when)
        def _():
            lax.fori_loop(EARLY_SLOPES, count, slopes, 0)

    for j in range(1, chunks):
        for copy in probe_copies(j):
            copy.wait_recv()
        for copy in forward(j):
            copy.start()
    later_slopes(crossing)
    for j in range(1, chunks):
        term_one(j)
    later_slopes(jnp.logical_not(crossing))

    def mate_copies(j):
        return [
            send(
                rest[j].at[e - 1, own],
                rest[j].at[e - 1, far_side],
                chip_s.at[e - 1, j],
                chip_r.at[e - 1, j],
                mate,
                q,
            )
            for e in range(1, wide)
        ]

    far_to = core * up + (1 - core) * down
    yonder = [
        send(
            rest[last].at[e - 1, pl.ds(count + half, half)],
            rest[last].at[e - 1, pl.ds((1 - core) * (2 * count) + half, half)],
            yonder_s.at[e - 1],
            yonder_r.at[e - 1],
            far_to,
            q,
        )
        for e in range(1, wide)
    ]

    for j in range(chunks):
        for copy, onward in zip(own_copies(j), mate_copies(j)):
            copy.wait_recv()
            onward.start()

    eye = (
        lax.broadcasted_iota(jnp.int32, (orbitals, orbitals), 0)
        == lax.broadcasted_iota(jnp.int32, (orbitals, orbitals), 1)
    ).astype(BF16)
    my_rows = pl.ds(pl.multiple_of(q * share, share), share)

    def mix_copies(j, c):
        copies = []
        for e in range(1, wide):
            to = lax.rem(q + e, wide)
            copies.append(
                send(
                    mix.at[j, c, pl.ds(pl.multiple_of(to * share, share), share)],
                    row_mix.at[j, q, c],
                    mix_s.at[e - 1, j, c],
                    mix_r.at[e - 1, j, c],
                    s,
                    to,
                )
            )
        return copies

    def term_two(j):
        def wait_one(c, carry):
            for copy in one_copies(j, c):
                copy.wait()
            return carry

        def body(c, carry):
            right = jnp.concatenate([one_t[j][slot_ref[c, k]] for k in range(slots)], axis=0)
            term = jnp.dot(scaled[c], right, preferred_element_type=F32)
            probe = lax.dot_general(
                eye, near[j][count + c], (((1,), (1,)), ((), ())), preferred_element_type=F32
            )
            second = 2.0 * term - probe
            mix[j, c] = (
                COEFF_ZERO * probe + COEFF_ONE * first[j, c] + COEFF_TWO * second
            ).astype(BF16)
            row_mix[j, q, c] = mix[j, c, my_rows, :]
            for copy in mix_copies(j, c):
                copy.start()
            return carry

        lax.fori_loop(0, count, wait_one, 0)
        if j == last:
            for copy in yonder:
                copy.start()
        lax.fori_loop(0, count, body, 0, unroll=4)

    def overlap(j):
        def wait_mix(c, carry):
            for copy in mix_copies(j, c):
                copy.wait()
            return carry

        def body(t, carry):
            left = jnp.concatenate(
                [row_mix[j, lax.rem(q + wide - w, wide)] for w in range(wide)], axis=2
            ).reshape(count * share, wide * width)
            right = jnp.concatenate(
                [
                    jnp.concatenate([source[2 * t], source[2 * t + 1]], axis=1)
                    for source in [near[j]] + [rest[j].at[w - 1] for w in range(1, wide)]
                ],
                axis=0,
            )
            product = jnp.dot(left, right, preferred_element_type=F32)
            for h in range(2):
                value = product[:, h * orbitals : (h + 1) * orbitals].reshape(
                    count, share, orbitals
                )
                dense[2 * t + h] = value if j == 0 else dense[2 * t + h] + value
            return carry

        for copy in forward(j) + mate_copies(j) + (yonder if j == last else []):
            copy.wait_recv()
        lax.fori_loop(0, count, wait_mix, 0)
        lax.fori_loop(0, 3 * count // 2, body, 0, unroll=4)

    for j in range(chunks):
        term_two(j)
    for j in range(chunks):
        overlap(j)

    padded = col_force.shape[1]

    def forces(c, carry):
        acc = [jnp.zeros((share, orbitals), F32) for _ in range(3)]
        for k in range(slots):
            sample = dense[slot_ref[c, k], c]
            for m in range(3):
                value = sample * slope[c, k, m]
                acc[m] = acc[m] + value
                col_force[c, k, m] = jnp.sum(
                    value.reshape(share // 8, 8, orbitals), axis=0
                )
        for m in range(3):
            row_force[m, c] = jnp.sum(acc[m].reshape(turns, height, orbitals), axis=0)
        return carry

    for k in range(slots, padded):
        for c in range(count):
            for m in range(3):
                col_force[c, k, m] = jnp.zeros((8, orbitals), F32)
    lax.fori_loop(0, count, forces, 0)

    ids = lax.broadcasted_iota(jnp.int32, (3 * count, slots), 0)
    held_ids = jnp.where(
        ids < count,
        ids + down * count,
        jnp.where(ids < 2 * count, ids - count + s * count, ids - 2 * count + up * count),
    )
    blank = jnp.zeros((3 * count, padded - slots), F32)
    picked = jnp.concatenate(
        [
            part
            for c in range(count)
            for part in (
                jnp.where(wanted_ref[c : c + 1, :] == held_ids, 1.0, 0.0),
                blank,
            )
        ],
        axis=1,
    )
    for m in range(3):
        column = jnp.sum(
            col_force[:, :, m].reshape(count * padded, 8, orbitals), axis=1
        )
        moved = jnp.dot(
            picked, column, precision=lax.Precision.HIGHEST, preferred_element_type=F32
        )
        pull[m] = fold(moved)
        line = jnp.sum(row_force[m], axis=2, keepdims=True) * hit
        pull[m, own] = pull[m, own] - jnp.sum(line, axis=1)
    arrived[1, q] = pull[:, own]
    pull_out = []
    for e in range(wide):
        to = lax.rem(q + e, wide)
        moves = [(pull.at[:, after], 0, up), (pull.at[:, before], 2, down)]
        if e > 0:
            moves.append((pull.at[:, own], 1, s))
        for src, kind, to_space in moves:
            copy = send(
                src, arrived.at[kind, q], pull_s.at[kind, e], pull_r.at[kind, e], to_space, to
            )
            copy.start()
            pull_out.append(copy)

    def density(k, carry):
        for c in range(count):
            sample = dense[slot_ref[c, k], c] * (alive_ref[c, k] * scale)
            stage[pl.ds(c, share, stride=count), :] = sample
        dens_ref[:, k] = stage[...].reshape(share, count, orbitals).astype(dens_ref.dtype)
        return carry

    lax.fori_loop(0, slots, density, 0)
    for copy in pull_out:
        copy.wait()
    result = None
    for kind in range(3):
        for w in range(wide):
            part = arrived[kind, w]
            result = part if result is None else result + part
    force_ref[...] = (result * (-1.0 / total))[:, :, :atoms]

    sent = [pos_up, pos_down] + yonder
    for j in range(chunks):
        sent = sent + probe_copies(j) + own_copies(j) + forward(j) + mate_copies(j)
    for copy in sent:
        copy.wait_send()


def write_out(pieces, dens_in, force_in, dens_out, force_out, sems):
    rows = dens_in.shape[0] // pieces
    copies = [pltpu.make_async_copy(force_in, force_out, sems.at[pieces])]
    for i in range(pieces):
        part = pl.ds(i * rows, rows)
        copies.append(pltpu.make_async_copy(dens_in.at[part], dens_out.at[part], sems.at[i]))
    for copy in copies:
        copy.start()
    for copy in copies:
        copy.wait()


def per_device(positions, probes, neighbours):
    count, _, atoms = positions.shape
    slots = neighbours.shape[1]
    orbitals = 4 * atoms
    span = probes.shape[1]
    space = lax.axis_size("space")
    wide = lax.axis_size("probe")
    share = orbitals // wide
    vmem = pl.BlockSpec(memory_space=pltpu.VMEM)
    dma = pltpu.SemaphoreType.DMA
    peers = max(wide - 1, 1)
    chunks = 2 if span % (2 * LANES) == 0 else 1
    plane = 2 ** ((space.bit_length() - 1) // 2)
    pairs = plane + space // plane - 2
    width = span // chunks
    sizes = (space, wide, count, atoms, slots, span, share, chunks, plane)
    density, force = pl.pallas_call(
        functools.partial(kernel, sizes),
        name="band_forces",
        out_shape=(
            pltpu.VMEM((share, slots, count, orbitals), BF16),
            pltpu.VMEM((3, count, atoms), F32),
        ),
        in_specs=[pl.BlockSpec(memory_space=pl.ANY)] * 3,
        out_specs=(vmem, vmem),
        scratch_shapes=[
            pltpu.SMEM((count, slots), jnp.int32),
            pltpu.SMEM((count, slots), jnp.int32),
            pltpu.SMEM((count, slots), F32),
            pltpu.VMEM((count, slots), jnp.int32),
            pltpu.VMEM((3, 3, count, atoms), BF16),
            pltpu.VMEM((count, 3, atoms, orbitals), F32),
            [pltpu.VMEM((3 * count, width, orbitals), BF16)] * chunks,
            [pltpu.VMEM((peers, 3 * count, width, orbitals), BF16)] * chunks,
            pltpu.VMEM((3, 3 * count, orbitals), F32),
            pltpu.VMEM((count, orbitals, slots * orbitals), F32),
            pltpu.VMEM((count, orbitals, slots * orbitals), BF16),
            pltpu.VMEM((count, slots, 7, atoms, orbitals), F32),
            pltpu.VMEM((2, 8, LANES), F32),
            pltpu.VMEM((pairs, 8, LANES), F32),
            pltpu.VMEM((count, slots, 3, share, orbitals), F32),
            pltpu.VMEM((chunks, count, orbitals, width), F32),
            [pltpu.VMEM((3 * count, orbitals, width), BF16)] * chunks,
            pltpu.VMEM((chunks, count, orbitals, width), BF16),
            pltpu.VMEM((chunks, wide, count, share, width), BF16),
            pltpu.VMEM((3 * count, count, share, orbitals), F32),
            pltpu.VMEM((share * count, orbitals), F32),
            pltpu.VMEM((count, -(-slots // 8) * 8, 3, 8, orbitals), F32),
            pltpu.VMEM((3, count, min(atoms, share), orbitals), F32),
            pltpu.VMEM((3, 3 * count, orbitals), F32),
            pltpu.VMEM((3, wide, 3, count, orbitals), F32),
            dma((3 + chunks,)),
            dma((2,)),
            dma((2,)),
            dma((2, chunks, 2)),
            dma((2, chunks, 2)),
            dma((peers, chunks)),
            dma((peers, chunks)),
            dma((peers, chunks)),
            dma((peers, chunks)),
            dma((peers, chunks)),
            dma((peers, chunks)),
            dma((peers,)),
            dma((peers,)),
            dma((pairs,)),
            dma((pairs,)),
            dma((2, chunks, count)),
            dma((2, chunks, count)),
            dma((peers, chunks, count)),
            dma((peers, chunks, count)),
            dma((3, wide)),
            dma((3, wide)),
        ],
        compiler_params=pltpu.CompilerParams(
            collective_id=0, has_side_effects=True, vmem_limit_bytes=60 * 1024 * 1024
        ),
    )(neighbours, jnp.transpose(positions, (1, 0, 2)), probes)
    anywhere = pl.BlockSpec(memory_space=pl.ANY)
    density, force = pl.pallas_call(
        functools.partial(write_out, PIECES),
        name="write_out",
        out_shape=(
            jax.ShapeDtypeStruct(density.shape, BF16),
            jax.ShapeDtypeStruct(force.shape, F32),
        ),
        in_specs=[vmem, vmem],
        out_specs=(anywhere, anywhere),
        scratch_shapes=[dma((PIECES + 1,))],
        compiler_params=pltpu.CompilerParams(vmem_limit_bytes=1024 * 1024),
    )(density, force)
    return jnp.transpose(density, (0, 2, 1, 3)), jnp.transpose(force, (1, 0, 2))


def solution(mesh):
    in_specs = (P("space", None, None), P("space", "probe", None), P("space", None))
    out_specs = (P("probe", "space", None, None), P("space", None, None))
    return jax.shard_map(
        per_device, mesh=mesh, in_specs=in_specs, out_specs=out_specs, check_vma=False
    )
```

```python
import functools

import jax
import jax.numpy as jnp
from jax import lax
from jax.experimental import pallas as pl
from jax.experimental.pallas import tpu as pltpu
from jax.sharding import PartitionSpec as P

SS_SIGMA = -1.938
SP_SIGMA = 1.745
PP_SIGMA = 3.05
PP_PI = -1.075
PP_DIFF = PP_SIGMA - PP_PI
BOND_LENGTH = 2.35
SOFT_SQUARE = 0.25
CELL_EDGE = 10.86
COEFF_ZERO = 0.6
COEFF_ONE = -0.7
COEFF_TWO = 0.45
MESH = pl.DeviceIdType.MESH
LANES = 128
F32 = jnp.float32
BF16 = jnp.bfloat16


def offsets():
    half = CELL_EDGE / 2.0
    table = [(0.0, 0.0, 0.0)]
    for x in (-1.0, 1.0):
        for y in (-1.0, 1.0):
            for z in (-1.0, 1.0):
                table.append((x * half, y * half, z * half))
    for axis in range(3):
        for sign in (1.0, -1.0):
            entry = [0.0, 0.0, 0.0]
            entry[axis] = sign * CELL_EDGE
            table.append(tuple(entry))
    return table


SHIFTS = offsets()
PIECES = 8
EARLY_BUILD = 2
EARLY_SLOPES = 0


def kernel(
    sizes,
    neighbours_ref,
    positions_ref,
    probes_ref,
    dens_ref,
    force_ref,
    names_ref,
    slot_ref,
    alive_ref,
    wanted_ref,
    raw_pos,
    posc_ref,
    near,
    rest,
    near_pos,
    ham,
    scaled,
    pair,
    top_out,
    top_in,
    slope,
    first,
    one_t,
    mix,
    row_mix,
    dense,
    stage,
    col_force,
    row_force,
    pull,
    arrived,
    local_sem,
    pos_s,
    pos_r,
    probe_s,
    probe_r,
    own_s,
    own_r,
    fwd_s,
    fwd_r,
    chip_s,
    chip_r,
    yonder_s,
    yonder_r,
    max_s,
    max_r,
    one_s,
    one_r,
    mix_s,
    mix_r,
    pull_s,
    pull_r,
):
    space, wide, count, atoms, slots, span, share, chunks, plane = sizes
    width = span // chunks
    orbitals = 4 * atoms
    total = span * wide
    s = lax.axis_index("space")
    q = lax.axis_index("probe")
    up = lax.rem(s + 1, space)
    down = lax.rem(s + space - 1, space)
    before, own, after = pl.ds(0, count), pl.ds(count, count), pl.ds(2 * count, count)
    core = lax.rem(s, 2)
    mate = s + 1 - 2 * core
    far_side = pl.ds(core * (2 * count), count)

    def send(src, dst, ss, rs, to_space, to_probe):
        return pltpu.make_async_remote_copy(
            src_ref=src,
            dst_ref=dst,
            send_sem=ss,
            recv_sem=rs,
            device_id={"space": to_space, "probe": to_probe},
            device_id_type=MESH,
        )

    low, high = lax.rem(s, plane), lax.div(s, plane)
    planes = space // plane
    beside = [high * plane + lax.rem(low + d, plane) for d in range(1, plane)]
    across = [lax.rem(high + d, planes) * plane + low for d in range(1, planes)]

    barrier = pltpu.get_barrier_semaphore()

    def greet(to_space, to_probe):
        pl.semaphore_signal(
            barrier,
            inc=1,
            device_id={"space": to_space, "probe": to_probe},
            device_id_type=MESH,
        )

    for to in beside + across + [up, down]:
        greet(to, q)
    for e in range(1, wide):
        greet(s, lax.rem(q + e, wide))

    loads = [
        pltpu.make_async_copy(src, dst, local_sem.at[i])
        for i, (src, dst) in enumerate(
            [
                (positions_ref, raw_pos.at[1]),
                (neighbours_ref, names_ref),
                (neighbours_ref, wanted_ref),
            ]
            + [
                (probes_ref.at[:, pl.ds(j * width, width)], near[j].at[own])
                for j in range(chunks)
            ]
        )
    ]
    for load in loads:
        load.start()
    pl.semaphore_wait(barrier, plane + planes + wide - 1)

    pos_up = send(positions_ref, raw_pos.at[0], pos_s.at[0], pos_r.at[0], up, q)
    pos_down = send(positions_ref, raw_pos.at[2], pos_s.at[1], pos_r.at[1], down, q)
    pos_up.start()
    pos_down.start()
    half = count // 2

    def probe_copies(j, halves=(0, 1)):
        part = pl.ds(j * width, width)
        return [
            send(
                probes_ref.at[pl.ds(h * half, half), part],
                near[j].at[pl.ds(place + h * half, half)],
                probe_s.at[i, j, h],
                probe_r.at[i, j, h],
                to,
                q,
            )
            for i, (place, to) in enumerate([(0, up), (2 * count, down)])
            for h in halves
        ]

    crossing = jnp.logical_or(lax.rem(s, 4) == 0, lax.rem(s, 4) == 3)

    def start_probes(when, j, halves=(0, 1)):
        @pl.when(when)
        def _():
            for copy in probe_copies(j, halves):
                copy.start()

    start_probes(jnp.logical_not(crossing), 0, (0,))
    def own_copies(j):
        return [
            send(
                probes_ref.at[:, pl.ds(j * width, width)],
                rest[j].at[e - 1, own],
                own_s.at[e - 1, j],
                own_r.at[e - 1, j],
                s,
                lax.rem(q + e, wide),
            )
            for e in range(1, wide)
        ]

    for copy in own_copies(0):
        copy.start()

    def fold(x):
        return (
            x
            + pltpu.roll(x, atoms, 1)
            + pltpu.roll(x, 2 * atoms, 1)
            + pltpu.roll(x, 3 * atoms, 1)
        )

    def spread(part):
        rows = pl.ds(part * count, count)
        for m in range(3):
            near_pos[m, rows, :atoms] = raw_pos[part, m].astype(F32)
            near_pos[m, rows] = fold(jnp.where(narrow, near_pos[m, rows], 0.0))

    for load in loads[:3]:
        load.wait()
    narrow = lax.broadcasted_iota(jnp.int32, (count, orbitals), 1) < atoms
    spread(1)
    for m in range(3):
        tall = jnp.transpose(near_pos[m, own])
        for c in range(count):
            posc_ref[c, m] = jnp.broadcast_to(tall[:atoms, c : c + 1], (atoms, orbitals))

    def find_slots(c, carry):
        for k in range(slots):
            name = names_ref[c, k]
            held = jnp.maximum(name, 0)
            place = lax.rem(lax.div(held, count) - s + 1 + space, space) * count
            place = place + lax.rem(held, count)
            slot_ref[c, k] = jnp.where(name >= 0, jnp.minimum(place, 3 * count - 1), count)
            alive_ref[c, k] = jnp.where(name >= 0, 1.0, 0.0)
        return carry

    lax.fori_loop(0, count, find_slots, 0)
    start_probes(crossing, 0)
    pos_up.wait_recv()
    spread(0)
    pos_down.wait_recv()
    spread(2)

    lane = lax.broadcasted_iota(jnp.int32, (atoms, orbitals), 1)
    group = lane // atoms
    is_s = group == 0
    is_p = [group == 1, group == 2, group == 3]
    pp = [jnp.where(m, PP_PI, 0.0).astype(F32) for m in is_p]

    def peak_of(c, peak):
        rows = [posc_ref[c, m] for m in range(3)]
        sums = [jnp.zeros((atoms, orbitals), F32) for _ in range(4)]
        for k in range(0, slots, 4):
            picked = range(k, min(k + 4, slots))
            alive = jnp.zeros((1, orbitals), F32)
            column = [jnp.zeros((1, orbitals), F32) for _ in range(3)]
            for i, t in enumerate(picked):
                here = group[:1] == i
                alive = jnp.where(here, alive_ref[c, t], alive)
                place = slot_ref[c, t]
                for m in range(3):
                    column[m] = jnp.where(
                        here, near_pos[m, pl.ds(place, 1), :] + SHIFTS[t][m], column[m]
                    )
            d = [column[m] - rows[m] for m in range(3)]
            square = d[0] * d[0] + d[1] * d[1] + d[2] * d[2] + SOFT_SQUARE
            inv = lax.rsqrt(square)
            u = [jnp.abs(x) * inv for x in d]
            g = jnp.exp(1.0 - square * (1.0 / (BOND_LENGTH * BOND_LENGTH))) * alive
            sums[0] = sums[0] + g * ((u[0] + u[1] + u[2]) * SP_SIGMA - SS_SIGMA)
            for a in range(3):
                others = u[(a + 1) % 3] + u[(a + 2) % 3]
                value = u[a] * (others * PP_DIFF + SP_SIGMA)
                value = value + jnp.abs(u[a] * u[a] * PP_DIFF + PP_PI)
                sums[1 + a] = sums[1 + a] + g * value
        for a in range(4):
            peak = jnp.maximum(peak, jnp.sum(sums[a], axis=1, keepdims=True))
        return peak

    def build(c, carry):
        rows = [posc_ref[c, m] for m in range(3)]
        for k in range(slots):
            place = slot_ref[c, k]
            alive = alive_ref[c, k]
            d = [
                (near_pos[m, pl.ds(place, 1), :] + SHIFTS[k][m]) - rows[m] for m in range(3)
            ]
            square = d[0] * d[0] + d[1] * d[1] + d[2] * d[2] + SOFT_SQUARE
            inv = lax.rsqrt(square)
            l = [x * inv for x in d]
            g = jnp.exp(1.0 - square * (1.0 / (BOND_LENGTH * BOND_LENGTH))) * alive
            beta = jnp.where(
                is_s, 0.0, jnp.where(is_p[0], l[0], jnp.where(is_p[1], l[1], l[2]))
            )
            coef_s = jnp.where(is_s, SS_SIGMA, SP_SIGMA * beta)
            coef_p = jnp.where(is_s, -SP_SIGMA, PP_DIFF * beta)
            parts = [coef_s * g] + [(l[m] * coef_p + pp[m]) * g for m in range(3)]
            for a in range(4):
                ham[c, a * atoms : (a + 1) * atoms, k * orbitals : (k + 1) * orbitals] = parts[a]
            pair[c, k, 0] = jnp.full_like(g, SP_SIGMA / PP_DIFF)
            for m in range(3):
                pair[c, k, 1 + m] = l[m]
            pair[c, k, 4] = coef_p
            pair[c, k, 5] = g * inv
            pair[c, k, 6] = square * inv * (2.0 / (BOND_LENGTH * BOND_LENGTH))
        return carry

    height = min(atoms, share)
    turns = share // height
    start_atom = lax.rem(q * share, atoms)
    rows = pl.ds(pl.multiple_of(start_atom, height), height)
    s_mask = jnp.where(is_s[:height], 1.0, 0.0).astype(F32)
    p_mask = [jnp.where(m[:height], 1.0, 0.0).astype(F32) for m in is_p]
    row_iota = lax.broadcasted_iota(jnp.int32, (height, orbitals), 0) + start_atom
    hit = jnp.where(row_iota == lax.rem(lane[:height], atoms), 1.0, 0.0).astype(F32)
    scale = 1.0 / float(total) ** 0.5

    def slopes(c, carry):
        for t in range(turns):
            kind = (q * share) // atoms + t
            is_row_p = jnp.where(kind > 0, 1.0, 0.0).astype(F32)
            plane_of = jnp.maximum(kind - 1, 0)
            twice = (1.0 + is_row_p) * (1.0 / PP_DIFF)
            lift = (SP_SIGMA / PP_DIFF) * s_mask
            own_rows = pl.ds(pl.multiple_of(q * share + t * height, height), height)
            part = slice(t * height, (t + 1) * height)
            for k in range(slots):
                c_two = pair[c, k, 4, rows, :]
                lean = pair[c, k, 5, rows, :]
                x = lean * (PP_DIFF * pair[c, k, kind, rows, :])
                y = lean * c_two
                block = ham[c, own_rows, k * orbitals : (k + 1) * orbitals]
                drag = x * (c_two * twice + lift) + block * pair[c, k, 6, rows, :]
                for m in range(3):
                    slope[c, k, m, part] = x * p_mask[m] - drag * pair[c, k, 1 + m, rows, :]
                slope[c, k, plane_of, part] = slope[c, k, plane_of, part] + y * is_row_p
        return carry

    peak = lax.fori_loop(0, count, peak_of, jnp.zeros((atoms, 1), F32), unroll=2)
    top = jnp.broadcast_to(jnp.max(peak, axis=0, keepdims=True), (8, LANES))

    def top_copies(stage, devices):
        base = 0 if stage == 0 else plane - 1
        return [
            send(
                top_out.at[stage],
                top_in.at[base + i],
                max_s.at[base + i],
                max_r.at[base + i],
                to,
                q,
            )
            for i, to in enumerate(devices)
        ]

    def raise_top(top, stage, devices):
        base = 0 if stage == 0 else plane - 1
        for i, copy in enumerate(top_copies(stage, devices)):
            copy.wait()
            top = jnp.maximum(top, top_in[base + i])
        return top

    last = chunks - 1

    def forward(j):
        copies = []
        far_part = pl.ds(core * (2 * count), half if j == last else count)
        for e in range(1, wide):
            copies.append(
                send(
                    near[j].at[far_part],
                    rest[j].at[e - 1, far_part],
                    fwd_s.at[e - 1, j],
                    fwd_r.at[e - 1, j],
                    s,
                    lax.rem(q + e, wide),
                )
            )
        return copies

    top_out[0] = top
    for copy in top_copies(0, beside):
        copy.start()
    start_probes(jnp.logical_not(crossing), 0, (1,))
    for j in range(1, chunks):
        start_probes(jnp.logical_not(crossing), j)
    for j in range(1, chunks):
        for copy in own_copies(j):
            copy.start()
    lax.fori_loop(0, EARLY_BUILD, build, 0)
    top = raise_top(top, 0, beside)
    top_out[1] = top
    for copy in top_copies(1, across):
        copy.start()
    for j in range(1, chunks):
        start_probes(crossing, j)
    lax.fori_loop(EARLY_BUILD, count, build, 0)
    lax.fori_loop(0, EARLY_SLOPES, slopes, 0)
    for load in loads[3:]:
        load.wait()
    for copy in probe_copies(0):
        copy.wait_recv()
    for copy in forward(0):
        copy.start()
    top = raise_top(top, 1, across)
    shrink = 1.0 / top[0:1]

    def one_copies(j, c):
        return [
            send(
                one_t[j].at[count + c],
                one_t[j].at[place + c],
                one_s.at[i, j, c],
                one_r.at[i, j, c],
                to,
                q,
            )
            for i, (place, to) in enumerate([(0, up), (2 * count, down)])
        ]

    def term_one(j):
        def body(c, carry):
            if j == 0:
                for k in range(slots):
                    here = pl.ds(k * orbitals, orbitals)
                    scaled[c, :, here] = (ham[c, :, here] * shrink).astype(BF16)
            right = jnp.concatenate([near[j][slot_ref[c, k]] for k in range(slots)], axis=1)
            term = lax.dot_general(
                scaled[c], right, (((1,), (1,)), ((), ())), preferred_element_type=F32
            )
            first[j, c] = term
            one_t[j][count + c] = term.astype(BF16)
            for copy in one_copies(j, c):
                copy.start()
            return carry

        lax.fori_loop(0, count, body, 0)

    term_one(0)
    def later_slopes(when):
        @pl.when(when)
        def _():
            lax.fori_loop(EARLY_SLOPES, count, slopes, 0)

    for j in range(1, chunks):
        for copy in probe_copies(j):
            copy.wait_recv()
        for copy in forward(j):
            copy.start()
    later_slopes(crossing)
    for j in range(1, chunks):
        term_one(j)
    later_slopes(jnp.logical_not(crossing))

    def mate_copies(j):
        return [
            send(
                rest[j].at[e - 1, own],
                rest[j].at[e - 1, far_side],
                chip_s.at[e - 1, j],
                chip_r.at[e - 1, j],
                mate,
                q,
            )
            for e in range(1, wide)
        ]

    far_to = core * up + (1 - core) * down
    yonder = [
        send(
            rest[last].at[e - 1, pl.ds(count + half, half)],
            rest[last].at[e - 1, pl.ds((1 - core) * (2 * count) + half, half)],
            yonder_s.at[e - 1],
            yonder_r.at[e - 1],
            far_to,
            q,
        )
        for e in range(1, wide)
    ]

    for j in range(chunks):
        for copy, onward in zip(own_copies(j), mate_copies(j)):
            copy.wait_recv()
            onward.start()

    eye = (
        lax.broadcasted_iota(jnp.int32, (orbitals, orbitals), 0)
        == lax.broadcasted_iota(jnp.int32, (orbitals, orbitals), 1)
    ).astype(BF16)
    my_rows = pl.ds(pl.multiple_of(q * share, share), share)

    def mix_copies(j, c):
        copies = []
        for e in range(1, wide):
            to = lax.rem(q + e, wide)
            copies.append(
                send(
                    mix.at[j, c, pl.ds(pl.multiple_of(to * share, share), share)],
                    row_mix.at[j, q, c],
                    mix_s.at[e - 1, j, c],
                    mix_r.at[e - 1, j, c],
                    s,
                    to,
                )
            )
        return copies

    def term_two(j):
        def wait_one(c, carry):
            for copy in one_copies(j, c):
                copy.wait()
            return carry

        def body(c, carry):
            right = jnp.concatenate([one_t[j][slot_ref[c, k]] for k in range(slots)], axis=0)
            term = jnp.dot(scaled[c], right, preferred_element_type=F32)
            probe = lax.dot_general(
                eye, near[j][count + c], (((1,), (1,)), ((), ())), preferred_element_type=F32
            )
            second = 2.0 * term - probe
            mix[j, c] = (
                COEFF_ZERO * probe + COEFF_ONE * first[j, c] + COEFF_TWO * second
            ).astype(BF16)
            row_mix[j, q, c] = mix[j, c, my_rows, :]
            for copy in mix_copies(j, c):
                copy.start()
            return carry

        lax.fori_loop(0, count, wait_one, 0)
        if j == last:
            for copy in yonder:
                copy.start()
        lax.fori_loop(0, count, body, 0, unroll=2)

    def overlap(j):
        def wait_mix(c, carry):
            for copy in mix_copies(j, c):
                copy.wait()
            return carry

        def body(t, carry):
            left = jnp.concatenate(
                [row_mix[j, lax.rem(q + wide - w, wide)] for w in range(wide)], axis=2
            ).reshape(count * share, wide * width)
            right = jnp.concatenate(
                [
                    jnp.concatenate([source[2 * t], source[2 * t + 1]], axis=1)
                    for source in [near[j]] + [rest[j].at[w - 1] for w in range(1, wide)]
                ],
                axis=0,
            )
            product = jnp.dot(left, right, preferred_element_type=F32)
            for h in range(2):
                value = product[:, h * orbitals : (h + 1) * orbitals].reshape(
                    count, share, orbitals
                )
                dense[2 * t + h] = value if j == 0 else dense[2 * t + h] + value
            return carry

        for copy in forward(j) + mate_copies(j) + (yonder if j == last else []):
            copy.wait_recv()
        lax.fori_loop(0, count, wait_mix, 0)
        lax.fori_loop(0, 3 * count // 2, body, 0, unroll=12)

    for j in range(chunks):
        term_two(j)
    for j in range(chunks):
        overlap(j)

    padded = col_force.shape[1]

    def forces(c, carry):
        acc = [jnp.zeros((share, orbitals), F32) for _ in range(3)]
        for k in range(slots):
            sample = dense[slot_ref[c, k], c]
            for m in range(3):
                value = sample * slope[c, k, m]
                acc[m] = acc[m] + value
                col_force[c, k, m] = jnp.sum(
                    value.reshape(share // 8, 8, orbitals), axis=0
                )
        for m in range(3):
            row_force[m, c] = jnp.sum(acc[m].reshape(turns, height, orbitals), axis=0)
        return carry

    for k in range(slots, padded):
        for c in range(count):
            for m in range(3):
                col_force[c, k, m] = jnp.zeros((8, orbitals), F32)
    lax.fori_loop(0, count, forces, 0, unroll=2)

    ids = lax.broadcasted_iota(jnp.int32, (3 * count, slots), 0)
    held_ids = jnp.where(
        ids < count,
        ids + down * count,
        jnp.where(ids < 2 * count, ids - count + s * count, ids - 2 * count + up * count),
    )
    blank = jnp.zeros((3 * count, padded - slots), F32)
    picked = jnp.concatenate(
        [
            part
            for c in range(count)
            for part in (
                jnp.where(wanted_ref[c : c + 1, :] == held_ids, 1.0, 0.0),
                blank,
            )
        ],
        axis=1,
    )
    for m in range(3):
        column = jnp.sum(
            col_force[:, :, m].reshape(count * padded, 8, orbitals), axis=1
        )
        moved = jnp.dot(
            picked, column, precision=lax.Precision.HIGHEST, preferred_element_type=F32
        )
        pull[m] = fold(moved)
        line = jnp.sum(row_force[m], axis=2, keepdims=True) * hit
        pull[m, own] = pull[m, own] - jnp.sum(line, axis=1)
    arrived[1, q] = pull[:, own]
    pull_out = []
    for e in range(wide):
        to = lax.rem(q + e, wide)
        moves = [(pull.at[:, after], 0, up), (pull.at[:, before], 2, down)]
        if e > 0:
            moves.append((pull.at[:, own], 1, s))
        for src, kind, to_space in moves:
            copy = send(
                src, arrived.at[kind, q], pull_s.at[kind, e], pull_r.at[kind, e], to_space, to
            )
            copy.start()
            pull_out.append(copy)

    def density(k, carry):
        for c in range(count):
            sample = dense[slot_ref[c, k], c] * (alive_ref[c, k] * scale)
            stage[pl.ds(c, share, stride=count), :] = sample
        dens_ref[:, k] = stage[...].reshape(share, count, orbitals).astype(dens_ref.dtype)
        return carry

    lax.fori_loop(0, slots, density, 0)
    for copy in pull_out:
        copy.wait()
    result = None
    for kind in range(3):
        for w in range(wide):
            part = arrived[kind, w]
            result = part if result is None else result + part
    force_ref[...] = (result * (-1.0 / total))[:, :, :atoms]

    sent = [pos_up, pos_down] + yonder
    for j in range(chunks):
        sent = sent + probe_copies(j) + own_copies(j) + forward(j) + mate_copies(j)
    for copy in sent:
        copy.wait_send()


def write_out(pieces, dens_in, force_in, dens_out, force_out, sems):
    rows = dens_in.shape[0] // pieces
    copies = [pltpu.make_async_copy(force_in, force_out, sems.at[pieces])]
    for i in range(pieces):
        part = pl.ds(i * rows, rows)
        copies.append(pltpu.make_async_copy(dens_in.at[part], dens_out.at[part], sems.at[i]))
    for copy in copies:
        copy.start()
    for copy in copies:
        copy.wait()


def per_device(positions, probes, neighbours):
    count, _, atoms = positions.shape
    slots = neighbours.shape[1]
    orbitals = 4 * atoms
    span = probes.shape[1]
    space = lax.axis_size("space")
    wide = lax.axis_size("probe")
    share = orbitals // wide
    vmem = pl.BlockSpec(memory_space=pltpu.VMEM)
    dma = pltpu.SemaphoreType.DMA
    peers = max(wide - 1, 1)
    chunks = 2 if span % (2 * LANES) == 0 else 1
    plane = 2 ** ((space.bit_length() - 1) // 2)
    pairs = plane + space // plane - 2
    width = span // chunks
    sizes = (space, wide, count, atoms, slots, span, share, chunks, plane)
    density, force = pl.pallas_call(
        functools.partial(kernel, sizes),
        name="band_forces",
        out_shape=(
            pltpu.VMEM((share, slots, count, orbitals), BF16),
            pltpu.VMEM((3, count, atoms), F32),
        ),
        in_specs=[pl.BlockSpec(memory_space=pl.ANY)] * 3,
        out_specs=(vmem, vmem),
        scratch_shapes=[
            pltpu.SMEM((count, slots), jnp.int32),
            pltpu.SMEM((count, slots), jnp.int32),
            pltpu.SMEM((count, slots), F32),
            pltpu.VMEM((count, slots), jnp.int32),
            pltpu.VMEM((3, 3, count, atoms), BF16),
            pltpu.VMEM((count, 3, atoms, orbitals), F32),
            [pltpu.VMEM((3 * count, width, orbitals), BF16)] * chunks,
            [pltpu.VMEM((peers, 3 * count, width, orbitals), BF16)] * chunks,
            pltpu.VMEM((3, 3 * count, orbitals), F32),
            pltpu.VMEM((count, orbitals, slots * orbitals), F32),
            pltpu.VMEM((count, orbitals, slots * orbitals), BF16),
            pltpu.VMEM((count, slots, 7, atoms, orbitals), F32),
            pltpu.VMEM((2, 8, LANES), F32),
            pltpu.VMEM((pairs, 8, LANES), F32),
            pltpu.VMEM((count, slots, 3, share, orbitals), F32),
            pltpu.VMEM((chunks, count, orbitals, width), F32),
            [pltpu.VMEM((3 * count, orbitals, width), BF16)] * chunks,
            pltpu.VMEM((chunks, count, orbitals, width), BF16),
            pltpu.VMEM((chunks, wide, count, share, width), BF16),
            pltpu.VMEM((3 * count, count, share, orbitals), F32),
            pltpu.VMEM((share * count, orbitals), F32),
            pltpu.VMEM((count, -(-slots // 8) * 8, 3, 8, orbitals), F32),
            pltpu.VMEM((3, count, min(atoms, share), orbitals), F32),
            pltpu.VMEM((3, 3 * count, orbitals), F32),
            pltpu.VMEM((3, wide, 3, count, orbitals), F32),
            dma((3 + chunks,)),
            dma((2,)),
            dma((2,)),
            dma((2, chunks, 2)),
            dma((2, chunks, 2)),
            dma((peers, chunks)),
            dma((peers, chunks)),
            dma((peers, chunks)),
            dma((peers, chunks)),
            dma((peers, chunks)),
            dma((peers, chunks)),
            dma((peers,)),
            dma((peers,)),
            dma((pairs,)),
            dma((pairs,)),
            dma((2, chunks, count)),
            dma((2, chunks, count)),
            dma((peers, chunks, count)),
            dma((peers, chunks, count)),
            dma((3, wide)),
            dma((3, wide)),
        ],
        compiler_params=pltpu.CompilerParams(
            collective_id=0, has_side_effects=True, vmem_limit_bytes=60 * 1024 * 1024
        ),
    )(neighbours, jnp.transpose(positions, (1, 0, 2)), probes)
    anywhere = pl.BlockSpec(memory_space=pl.ANY)
    density, force = pl.pallas_call(
        functools.partial(write_out, PIECES),
        name="write_out",
        out_shape=(
            jax.ShapeDtypeStruct(density.shape, BF16),
            jax.ShapeDtypeStruct(force.shape, F32),
        ),
        in_specs=[vmem, vmem],
        out_specs=(anywhere, anywhere),
        scratch_shapes=[dma((PIECES + 1,))],
        compiler_params=pltpu.CompilerParams(vmem_limit_bytes=1024 * 1024),
    )(density, force)
    return jnp.transpose(density, (0, 2, 1, 3)), jnp.transpose(force, (1, 0, 2))


def solution(mesh):
    in_specs = (P("space", None, None), P("space", "probe", None), P("space", None))
    out_specs = (P("probe", "space", None, None), P("space", None, None))
    return jax.shard_map(
        per_device, mesh=mesh, in_specs=in_specs, out_specs=out_specs, check_vma=False
    )
```

```python
import functools

import jax
import jax.numpy as jnp
from jax import lax
from jax.experimental import pallas as pl
from jax.experimental.pallas import tpu as pltpu
from jax.sharding import PartitionSpec as P

SS_SIGMA = -1.938
SP_SIGMA = 1.745
PP_SIGMA = 3.05
PP_PI = -1.075
PP_DIFF = PP_SIGMA - PP_PI
BOND_LENGTH = 2.35
SOFT_SQUARE = 0.25
CELL_EDGE = 10.86
COEFF_ZERO = 0.6
COEFF_ONE = -0.7
COEFF_TWO = 0.45
MESH = pl.DeviceIdType.MESH
LANES = 128
F32 = jnp.float32
BF16 = jnp.bfloat16


def offsets():
    half = CELL_EDGE / 2.0
    table = [(0.0, 0.0, 0.0)]
    for x in (-1.0, 1.0):
        for y in (-1.0, 1.0):
            for z in (-1.0, 1.0):
                table.append((x * half, y * half, z * half))
    for axis in range(3):
        for sign in (1.0, -1.0):
            entry = [0.0, 0.0, 0.0]
            entry[axis] = sign * CELL_EDGE
            table.append(tuple(entry))
    return table


SHIFTS = offsets()
PIECES = 8
EARLY_BUILD = 2
EARLY_SLOPES = 0


def kernel(
    sizes,
    neighbours_ref,
    positions_ref,
    probes_ref,
    dens_ref,
    force_ref,
    names_ref,
    slot_ref,
    alive_ref,
    wanted_ref,
    raw_pos,
    posc_ref,
    near,
    rest,
    near_pos,
    ham,
    scaled,
    pair,
    top_out,
    top_in,
    slope,
    first,
    one_t,
    mix,
    row_mix,
    dense,
    stage,
    col_force,
    row_force,
    pull,
    arrived,
    local_sem,
    pos_s,
    pos_r,
    probe_s,
    probe_r,
    own_s,
    own_r,
    fwd_s,
    fwd_r,
    chip_s,
    chip_r,
    yonder_s,
    yonder_r,
    max_s,
    max_r,
    one_s,
    one_r,
    mix_s,
    mix_r,
    pull_s,
    pull_r,
):
    space, wide, count, atoms, slots, span, share, chunks, plane = sizes
    width = span // chunks
    orbitals = 4 * atoms
    total = span * wide
    s = lax.axis_index("space")
    q = lax.axis_index("probe")
    up = lax.rem(s + 1, space)
    down = lax.rem(s + space - 1, space)
    before, own, after = pl.ds(0, count), pl.ds(count, count), pl.ds(2 * count, count)
    core = lax.rem(s, 2)
    mate = s + 1 - 2 * core
    far_side = pl.ds(core * (2 * count), count)

    def send(src, dst, ss, rs, to_space, to_probe):
        return pltpu.make_async_remote_copy(
            src_ref=src,
            dst_ref=dst,
            send_sem=ss,
            recv_sem=rs,
            device_id={"space": to_space, "probe": to_probe},
            device_id_type=MESH,
        )

    low, high = lax.rem(s, plane), lax.div(s, plane)
    planes = space // plane
    beside = [high * plane + lax.rem(low + d, plane) for d in range(1, plane)]
    across = [lax.rem(high + d, planes) * plane + low for d in range(1, planes)]

    barrier = pltpu.get_barrier_semaphore()

    def greet(to_space, to_probe):
        pl.semaphore_signal(
            barrier,
            inc=1,
            device_id={"space": to_space, "probe": to_probe},
            device_id_type=MESH,
        )

    for to in beside + across + [up, down]:
        greet(to, q)
    for e in range(1, wide):
        greet(s, lax.rem(q + e, wide))

    loads = [
        pltpu.make_async_copy(src, dst, local_sem.at[i])
        for i, (src, dst) in enumerate(
            [
                (positions_ref, raw_pos.at[1]),
                (neighbours_ref, names_ref),
                (neighbours_ref, wanted_ref),
            ]
            + [
                (probes_ref.at[:, pl.ds(j * width, width)], near[j].at[own])
                for j in range(chunks)
            ]
        )
    ]
    for load in loads:
        load.start()
    pl.semaphore_wait(barrier, plane + planes + wide - 1)

    pos_up = send(positions_ref, raw_pos.at[0], pos_s.at[0], pos_r.at[0], up, q)
    pos_down = send(positions_ref, raw_pos.at[2], pos_s.at[1], pos_r.at[1], down, q)
    pos_up.start()
    pos_down.start()
    half = count // 2

    def probe_copies(j, halves=(0, 1)):
        part = pl.ds(j * width, width)
        return [
            send(
                probes_ref.at[pl.ds(h * half, half), part],
                near[j].at[pl.ds(place + h * half, half)],
                probe_s.at[i, j, h],
                probe_r.at[i, j, h],
                to,
                q,
            )
            for i, (place, to) in enumerate([(0, up), (2 * count, down)])
            for h in halves
        ]

    crossing = jnp.logical_or(lax.rem(s, 4) == 0, lax.rem(s, 4) == 3)

    def start_probes(when, j, halves=(0, 1)):
        @pl.when(when)
        def _():
            for copy in probe_copies(j, halves):
                copy.start()

    start_probes(jnp.logical_not(crossing), 0, (0,))
    def own_copies(j):
        return [
            send(
                probes_ref.at[:, pl.ds(j * width, width)],
                rest[j].at[e - 1, own],
                own_s.at[e - 1, j],
                own_r.at[e - 1, j],
                s,
                lax.rem(q + e, wide),
            )
            for e in range(1, wide)
        ]

    for copy in own_copies(0):
        copy.start()

    def fold(x):
        return (
            x
            + pltpu.roll(x, atoms, 1)
            + pltpu.roll(x, 2 * atoms, 1)
            + pltpu.roll(x, 3 * atoms, 1)
        )

    def spread(part):
        rows = pl.ds(part * count, count)
        for m in range(3):
            near_pos[m, rows, :atoms] = raw_pos[part, m].astype(F32)
            near_pos[m, rows] = fold(jnp.where(narrow, near_pos[m, rows], 0.0))

    for load in loads[:3]:
        load.wait()
    narrow = lax.broadcasted_iota(jnp.int32, (count, orbitals), 1) < atoms
    spread(1)
    for m in range(3):
        tall = jnp.transpose(near_pos[m, own])
        for c in range(count):
            posc_ref[c, m] = jnp.broadcast_to(tall[:atoms, c : c + 1], (atoms, orbitals))

    def find_slots(c, carry):
        for k in range(slots):
            name = names_ref[c, k]
            held = jnp.maximum(name, 0)
            place = lax.rem(lax.div(held, count) - s + 1 + space, space) * count
            place = place + lax.rem(held, count)
            slot_ref[c, k] = jnp.where(name >= 0, jnp.minimum(place, 3 * count - 1), count)
            alive_ref[c, k] = jnp.where(name >= 0, 1.0, 0.0)
        return carry

    lax.fori_loop(0, count, find_slots, 0)
    start_probes(crossing, 0)
    pos_up.wait_recv()
    spread(0)
    pos_down.wait_recv()
    spread(2)

    lane = lax.broadcasted_iota(jnp.int32, (atoms, orbitals), 1)
    group = lane // atoms
    is_s = group == 0
    is_p = [group == 1, group == 2, group == 3]
    pp = [jnp.where(m, PP_PI, 0.0).astype(F32) for m in is_p]

    def peak_of(c, peak):
        rows = [posc_ref[c, m] for m in range(3)]
        sums = [jnp.zeros((atoms, orbitals), F32) for _ in range(4)]
        for k in range(0, slots, 4):
            picked = range(k, min(k + 4, slots))
            alive = jnp.zeros((1, orbitals), F32)
            column = [jnp.zeros((1, orbitals), F32) for _ in range(3)]
            for i, t in enumerate(picked):
                here = group[:1] == i
                alive = jnp.where(here, alive_ref[c, t], alive)
                place = slot_ref[c, t]
                for m in range(3):
                    column[m] = jnp.where(
                        here, near_pos[m, pl.ds(place, 1), :] + SHIFTS[t][m], column[m]
                    )
            d = [column[m] - rows[m] for m in range(3)]
            square = d[0] * d[0] + d[1] * d[1] + d[2] * d[2] + SOFT_SQUARE
            inv = lax.rsqrt(square)
            u = [jnp.abs(x) * inv for x in d]
            g = jnp.exp(1.0 - square * (1.0 / (BOND_LENGTH * BOND_LENGTH))) * alive
            sums[0] = sums[0] + g * ((u[0] + u[1] + u[2]) * SP_SIGMA - SS_SIGMA)
            for a in range(3):
                others = u[(a + 1) % 3] + u[(a + 2) % 3]
                value = u[a] * (others * PP_DIFF + SP_SIGMA)
                value = value + jnp.abs(u[a] * u[a] * PP_DIFF + PP_PI)
                sums[1 + a] = sums[1 + a] + g * value
        for a in range(4):
            peak = jnp.maximum(peak, jnp.sum(sums[a], axis=1, keepdims=True))
        return peak

    def build(c, carry):
        rows = [posc_ref[c, m] for m in range(3)]
        for k in range(slots):
            place = slot_ref[c, k]
            alive = alive_ref[c, k]
            d = [
                (near_pos[m, pl.ds(place, 1), :] + SHIFTS[k][m]) - rows[m] for m in range(3)
            ]
            square = d[0] * d[0] + d[1] * d[1] + d[2] * d[2] + SOFT_SQUARE
            inv = lax.rsqrt(square)
            l = [x * inv for x in d]
            g = jnp.exp(1.0 - square * (1.0 / (BOND_LENGTH * BOND_LENGTH))) * alive
            beta = jnp.where(
                is_s, 0.0, jnp.where(is_p[0], l[0], jnp.where(is_p[1], l[1], l[2]))
            )
            coef_s = jnp.where(is_s, SS_SIGMA, SP_SIGMA * beta)
            coef_p = jnp.where(is_s, -SP_SIGMA, PP_DIFF * beta)
            parts = [coef_s * g] + [(l[m] * coef_p + pp[m]) * g for m in range(3)]
            for a in range(4):
                ham[c, a * atoms : (a + 1) * atoms, k * orbitals : (k + 1) * orbitals] = parts[a]
            pair[c, k, 0] = jnp.full_like(g, SP_SIGMA / PP_DIFF)
            for m in range(3):
                pair[c, k, 1 + m] = l[m]
            pair[c, k, 4] = coef_p
            pair[c, k, 5] = g * inv
            pair[c, k, 6] = square * inv * (2.0 / (BOND_LENGTH * BOND_LENGTH))
        return carry

    height = min(atoms, share)
    turns = share // height
    start_atom = lax.rem(q * share, atoms)
    rows = pl.ds(pl.multiple_of(start_atom, height), height)
    s_mask = jnp.where(is_s[:height], 1.0, 0.0).astype(F32)
    p_mask = [jnp.where(m[:height], 1.0, 0.0).astype(F32) for m in is_p]
    row_iota = lax.broadcasted_iota(jnp.int32, (height, orbitals), 0) + start_atom
    hit = jnp.where(row_iota == lax.rem(lane[:height], atoms), 1.0, 0.0).astype(F32)
    scale = 1.0 / float(total) ** 0.5

    def slopes(c, carry):
        for t in range(turns):
            kind = (q * share) // atoms + t
            is_row_p = jnp.where(kind > 0, 1.0, 0.0).astype(F32)
            plane_of = jnp.maximum(kind - 1, 0)
            twice = (1.0 + is_row_p) * (1.0 / PP_DIFF)
            lift = (SP_SIGMA / PP_DIFF) * s_mask
            own_rows = pl.ds(pl.multiple_of(q * share + t * height, height), height)
            part = slice(t * height, (t + 1) * height)
            for k in range(slots):
                c_two = pair[c, k, 4, rows, :]
                lean = pair[c, k, 5, rows, :]
                x = lean * (PP_DIFF * pair[c, k, kind, rows, :])
                y = lean * c_two
                block = ham[c, own_rows, k * orbitals : (k + 1) * orbitals]
                drag = x * (c_two * twice + lift) + block * pair[c, k, 6, rows, :]
                for m in range(3):
                    slope[c, k, m, part] = x * p_mask[m] - drag * pair[c, k, 1 + m, rows, :]
                slope[c, k, plane_of, part] = slope[c, k, plane_of, part] + y * is_row_p
        return carry

    peak = lax.fori_loop(0, count, peak_of, jnp.zeros((atoms, 1), F32), unroll=4)
    top = jnp.broadcast_to(jnp.max(peak, axis=0, keepdims=True), (8, LANES))

    def top_copies(stage, devices):
        base = 0 if stage == 0 else plane - 1
        return [
            send(
                top_out.at[stage],
                top_in.at[base + i],
                max_s.at[base + i],
                max_r.at[base + i],
                to,
                q,
            )
            for i, to in enumerate(devices)
        ]

    def raise_top(top, stage, devices):
        base = 0 if stage == 0 else plane - 1
        for i, copy in enumerate(top_copies(stage, devices)):
            copy.wait()
            top = jnp.maximum(top, top_in[base + i])
        return top

    last = chunks - 1

    def forward(j):
        copies = []
        far_part = pl.ds(core * (2 * count), half if j == last else count)
        for e in range(1, wide):
            copies.append(
                send(
                    near[j].at[far_part],
                    rest[j].at[e - 1, far_part],
                    fwd_s.at[e - 1, j],
                    fwd_r.at[e - 1, j],
                    s,
                    lax.rem(q + e, wide),
                )
            )
        return copies

    top_out[0] = top
    for copy in top_copies(0, beside):
        copy.start()
    start_probes(jnp.logical_not(crossing), 0, (1,))
    for j in range(1, chunks):
        start_probes(jnp.logical_not(crossing), j)
    for j in range(1, chunks):
        for copy in own_copies(j):
            copy.start()
    lax.fori_loop(0, EARLY_BUILD, build, 0)
    top = raise_top(top, 0, beside)
    top_out[1] = top
    for copy in top_copies(1, across):
        copy.start()
    for j in range(1, chunks):
        start_probes(crossing, j)
    lax.fori_loop(EARLY_BUILD, count, build, 0)
    lax.fori_loop(0, EARLY_SLOPES, slopes, 0)
    for load in loads[3:]:
        load.wait()
    for copy in probe_copies(0):
        copy.wait_recv()
    for copy in forward(0):
        copy.start()
    top = raise_top(top, 1, across)
    shrink = 1.0 / top[0:1]

    def one_copies(j, c):
        return [
            send(
                one_t[j].at[count + c],
                one_t[j].at[place + c],
                one_s.at[i, j, c],
                one_r.at[i, j, c],
                to,
                q,
            )
            for i, (place, to) in enumerate([(0, up), (2 * count, down)])
        ]

    def term_one(j):
        def body(c, carry):
            if j == 0:
                for k in range(slots):
                    here = pl.ds(k * orbitals, orbitals)
                    scaled[c, :, here] = (ham[c, :, here] * shrink).astype(BF16)
            right = jnp.concatenate([near[j][slot_ref[c, k]] for k in range(slots)], axis=1)
            term = lax.dot_general(
                scaled[c], right, (((1,), (1,)), ((), ())), preferred_element_type=F32
            )
            first[j, c] = term
            one_t[j][count + c] = term.astype(BF16)
            for copy in one_copies(j, c):
                copy.start()
            return carry

        lax.fori_loop(0, count, body, 0)

    term_one(0)
    def later_slopes(when):
        @pl.when(when)
        def _():
            lax.fori_loop(EARLY_SLOPES, count, slopes, 0)

    for j in range(1, chunks):
        for copy in probe_copies(j):
            copy.wait_recv()
        for copy in forward(j):
            copy.start()
    later_slopes(crossing)
    for j in range(1, chunks):
        term_one(j)
    later_slopes(jnp.logical_not(crossing))

    def mate_copies(j):
        return [
            send(
                rest[j].at[e - 1, own],
                rest[j].at[e - 1, far_side],
                chip_s.at[e - 1, j],
                chip_r.at[e - 1, j],
                mate,
                q,
            )
            for e in range(1, wide)
        ]

    far_to = core * up + (1 - core) * down
    yonder = [
        send(
            rest[last].at[e - 1, pl.ds(count + half, half)],
            rest[last].at[e - 1, pl.ds((1 - core) * (2 * count) + half, half)],
            yonder_s.at[e - 1],
            yonder_r.at[e - 1],
            far_to,
            q,
        )
        for e in range(1, wide)
    ]

    for j in range(chunks):
        for copy, onward in zip(own_copies(j), mate_copies(j)):
            copy.wait_recv()
            onward.start()

    eye = (
        lax.broadcasted_iota(jnp.int32, (orbitals, orbitals), 0)
        == lax.broadcasted_iota(jnp.int32, (orbitals, orbitals), 1)
    ).astype(BF16)
    my_rows = pl.ds(pl.multiple_of(q * share, share), share)

    def mix_copies(j, c):
        copies = []
        for e in range(1, wide):
            to = lax.rem(q + e, wide)
            copies.append(
                send(
                    mix.at[j, c, pl.ds(pl.multiple_of(to * share, share), share)],
                    row_mix.at[j, q, c],
                    mix_s.at[e - 1, j, c],
                    mix_r.at[e - 1, j, c],
                    s,
                    to,
                )
            )
        return copies

    def term_two(j):
        def wait_one(c, carry):
            for copy in one_copies(j, c):
                copy.wait()
            return carry

        def body(c, carry):
            right = jnp.concatenate([one_t[j][slot_ref[c, k]] for k in range(slots)], axis=0)
            term = jnp.dot(scaled[c], right, preferred_element_type=F32)
            probe = lax.dot_general(
                eye, near[j][count + c], (((1,), (1,)), ((), ())), preferred_element_type=F32
            )
            second = 2.0 * term - probe
            mix[j, c] = (
                COEFF_ZERO * probe + COEFF_ONE * first[j, c] + COEFF_TWO * second
            ).astype(BF16)
            row_mix[j, q, c] = mix[j, c, my_rows, :]
            for copy in mix_copies(j, c):
                copy.start()
            return carry

        lax.fori_loop(0, count, wait_one, 0)
        if j == last:
            for copy in yonder:
                copy.start()
        lax.fori_loop(0, count, body, 0, unroll=2)

    def overlap(j):
        def wait_mix(c, carry):
            for copy in mix_copies(j, c):
                copy.wait()
            return carry

        def body(t, carry):
            left = jnp.concatenate(
                [row_mix[j, lax.rem(q + wide - w, wide)] for w in range(wide)], axis=2
            ).reshape(count * share, wide * width)
            right = jnp.concatenate(
                [
                    jnp.concatenate([source[2 * t], source[2 * t + 1]], axis=1)
                    for source in [near[j]] + [rest[j].at[w - 1] for w in range(1, wide)]
                ],
                axis=0,
            )
            product = jnp.dot(left, right, preferred_element_type=F32)
            for h in range(2):
                value = product[:, h * orbitals : (h + 1) * orbitals].reshape(
                    count, share, orbitals
                )
                dense[2 * t + h] = value if j == 0 else dense[2 * t + h] + value
            return carry

        for copy in forward(j) + mate_copies(j) + (yonder if j == last else []):
            copy.wait_recv()
        lax.fori_loop(0, count, wait_mix, 0)
        lax.fori_loop(0, 3 * count // 2, body, 0, unroll=12)

    for j in range(chunks):
        term_two(j)
    for j in range(chunks):
        overlap(j)

    padded = col_force.shape[1]

    def forces(c, carry):
        acc = [jnp.zeros((share, orbitals), F32) for _ in range(3)]
        for k in range(slots):
            sample = dense[slot_ref[c, k], c]
            for m in range(3):
                value = sample * slope[c, k, m]
                acc[m] = acc[m] + value
                col_force[c, k, m] = jnp.sum(
                    value.reshape(share // 8, 8, orbitals), axis=0
                )
        for m in range(3):
            row_force[m, c] = jnp.sum(acc[m].reshape(turns, height, orbitals), axis=0)
        return carry

    for k in range(slots, padded):
        for c in range(count):
            for m in range(3):
                col_force[c, k, m] = jnp.zeros((8, orbitals), F32)
    lax.fori_loop(0, count, forces, 0, unroll=2)

    ids = lax.broadcasted_iota(jnp.int32, (3 * count, slots), 0)
    held_ids = jnp.where(
        ids < count,
        ids + down * count,
        jnp.where(ids < 2 * count, ids - count + s * count, ids - 2 * count + up * count),
    )
    blank = jnp.zeros((3 * count, padded - slots), F32)
    picked = jnp.concatenate(
        [
            part
            for c in range(count)
            for part in (
                jnp.where(wanted_ref[c : c + 1, :] == held_ids, 1.0, 0.0),
                blank,
            )
        ],
        axis=1,
    )
    for m in range(3):
        column = jnp.sum(
            col_force[:, :, m].reshape(count * padded, 8, orbitals), axis=1
        )
        moved = jnp.dot(
            picked, column, precision=lax.Precision.HIGHEST, preferred_element_type=F32
        )
        pull[m] = fold(moved)
        line = jnp.sum(row_force[m], axis=2, keepdims=True) * hit
        pull[m, own] = pull[m, own] - jnp.sum(line, axis=1)
    arrived[1, q] = pull[:, own]
    pull_out = []
    for e in range(wide):
        to = lax.rem(q + e, wide)
        moves = [(pull.at[:, after], 0, up), (pull.at[:, before], 2, down)]
        if e > 0:
            moves.append((pull.at[:, own], 1, s))
        for src, kind, to_space in moves:
            copy = send(
                src, arrived.at[kind, q], pull_s.at[kind, e], pull_r.at[kind, e], to_space, to
            )
            copy.start()
            pull_out.append(copy)

    def density(k, carry):
        for c in range(count):
            sample = dense[slot_ref[c, k], c] * (alive_ref[c, k] * scale)
            stage[pl.ds(c, share, stride=count), :] = sample
        dens_ref[:, k] = stage[...].reshape(share, count, orbitals).astype(dens_ref.dtype)
        return carry

    lax.fori_loop(0, slots, density, 0)
    for copy in pull_out:
        copy.wait()
    result = None
    for kind in range(3):
        for w in range(wide):
            part = arrived[kind, w]
            result = part if result is None else result + part
    force_ref[...] = (result * (-1.0 / total))[:, :, :atoms]

    sent = [pos_up, pos_down] + yonder
    for j in range(chunks):
        sent = sent + probe_copies(j) + own_copies(j) + forward(j) + mate_copies(j)
    for copy in sent:
        copy.wait_send()


def write_out(pieces, dens_in, force_in, dens_out, force_out, sems):
    rows = dens_in.shape[0] // pieces
    copies = [pltpu.make_async_copy(force_in, force_out, sems.at[pieces])]
    for i in range(pieces):
        part = pl.ds(i * rows, rows)
        copies.append(pltpu.make_async_copy(dens_in.at[part], dens_out.at[part], sems.at[i]))
    for copy in copies:
        copy.start()
    for copy in copies:
        copy.wait()


def per_device(positions, probes, neighbours):
    count, _, atoms = positions.shape
    slots = neighbours.shape[1]
    orbitals = 4 * atoms
    span = probes.shape[1]
    space = lax.axis_size("space")
    wide = lax.axis_size("probe")
    share = orbitals // wide
    vmem = pl.BlockSpec(memory_space=pltpu.VMEM)
    dma = pltpu.SemaphoreType.DMA
    peers = max(wide - 1, 1)
    chunks = 2 if span % (2 * LANES) == 0 else 1
    plane = 2 ** ((space.bit_length() - 1) // 2)
    pairs = plane + space // plane - 2
    width = span // chunks
    sizes = (space, wide, count, atoms, slots, span, share, chunks, plane)
    density, force = pl.pallas_call(
        functools.partial(kernel, sizes),
        name="band_forces",
        out_shape=(
            pltpu.VMEM((share, slots, count, orbitals), BF16),
            pltpu.VMEM((3, count, atoms), F32),
        ),
        in_specs=[pl.BlockSpec(memory_space=pl.ANY)] * 3,
        out_specs=(vmem, vmem),
        scratch_shapes=[
            pltpu.SMEM((count, slots), jnp.int32),
            pltpu.SMEM((count, slots), jnp.int32),
            pltpu.SMEM((count, slots), F32),
            pltpu.VMEM((count, slots), jnp.int32),
            pltpu.VMEM((3, 3, count, atoms), BF16),
            pltpu.VMEM((count, 3, atoms, orbitals), F32),
            [pltpu.VMEM((3 * count, width, orbitals), BF16)] * chunks,
            [pltpu.VMEM((peers, 3 * count, width, orbitals), BF16)] * chunks,
            pltpu.VMEM((3, 3 * count, orbitals), F32),
            pltpu.VMEM((count, orbitals, slots * orbitals), F32),
            pltpu.VMEM((count, orbitals, slots * orbitals), BF16),
            pltpu.VMEM((count, slots, 7, atoms, orbitals), F32),
            pltpu.VMEM((2, 8, LANES), F32),
            pltpu.VMEM((pairs, 8, LANES), F32),
            pltpu.VMEM((count, slots, 3, share, orbitals), F32),
            pltpu.VMEM((chunks, count, orbitals, width), F32),
            [pltpu.VMEM((3 * count, orbitals, width), BF16)] * chunks,
            pltpu.VMEM((chunks, count, orbitals, width), BF16),
            pltpu.VMEM((chunks, wide, count, share, width), BF16),
            pltpu.VMEM((3 * count, count, share, orbitals), F32),
            pltpu.VMEM((share * count, orbitals), F32),
            pltpu.VMEM((count, -(-slots // 8) * 8, 3, 8, orbitals), F32),
            pltpu.VMEM((3, count, min(atoms, share), orbitals), F32),
            pltpu.VMEM((3, 3 * count, orbitals), F32),
            pltpu.VMEM((3, wide, 3, count, orbitals), F32),
            dma((3 + chunks,)),
            dma((2,)),
            dma((2,)),
            dma((2, chunks, 2)),
            dma((2, chunks, 2)),
            dma((peers, chunks)),
            dma((peers, chunks)),
            dma((peers, chunks)),
            dma((peers, chunks)),
            dma((peers, chunks)),
            dma((peers, chunks)),
            dma((peers,)),
            dma((peers,)),
            dma((pairs,)),
            dma((pairs,)),
            dma((2, chunks, count)),
            dma((2, chunks, count)),
            dma((peers, chunks, count)),
            dma((peers, chunks, count)),
            dma((3, wide)),
            dma((3, wide)),
        ],
        compiler_params=pltpu.CompilerParams(
            collective_id=0, has_side_effects=True, vmem_limit_bytes=60 * 1024 * 1024
        ),
    )(neighbours, jnp.transpose(positions, (1, 0, 2)), probes)
    anywhere = pl.BlockSpec(memory_space=pl.ANY)
    density, force = pl.pallas_call(
        functools.partial(write_out, PIECES),
        name="write_out",
        out_shape=(
            jax.ShapeDtypeStruct(density.shape, BF16),
            jax.ShapeDtypeStruct(force.shape, F32),
        ),
        in_specs=[vmem, vmem],
        out_specs=(anywhere, anywhere),
        scratch_shapes=[dma((PIECES + 1,))],
        compiler_params=pltpu.CompilerParams(vmem_limit_bytes=1024 * 1024),
    )(density, force)
    return jnp.transpose(density, (0, 2, 1, 3)), jnp.transpose(force, (1, 0, 2))


def solution(mesh):
    in_specs = (P("space", None, None), P("space", "probe", None), P("space", None))
    out_specs = (P("probe", "space", None, None), P("space", None, None))
    return jax.shard_map(
        per_device, mesh=mesh, in_specs=in_specs, out_specs=out_specs, check_vma=False
    )
```
